256 devices in a mesh: prow: 16 (over y, x), pcol: 16 (over z, core).
Axes of the slice: x: 4, y: 4, z: 8, core: 2. Of those that a mesh axis runs over, the one named last changes fastest.
Arguments:
- blocked: float32 [16384, 16384], P('prow', 'pcol'), may hold values from -6 to 6, as said below
Outputs:
- factored: float32 [16384, 16384], P('prow', 'pcol')
The draws below stay inside these ranges and needn't reach their ends.
Inputs may be any that keep to these rules, and one draw needn't show every extreme that they name: blocked is the block-cyclic storage of a symmetric positive definite matrix whose diagonal is at least 1 plus a nonnegative Gram diagonal and whose condition number is below about 40.
All inputs are finite; a program needn't handle non-finite values.
Results may differ from the reference program's by a relative error of at most 0.0003.
Values sent between devices are 32-bit elements.
A program may use at most 128 MiB of HBM per device.

```python
import jax
import jax.numpy as jnp
from jax import lax

EMB = 2048
BLOCK = 128
STEPS = 8
N = 16384
N_PROW = 16
N_PCOL = 16


def draw_blocked(key, part):
    first_key, second_key = jax.random.split(jax.random.fold_in(key, 7))
    features = jax.random.normal(first_key, (N, EMB), jnp.float32)
    gram = jnp.dot(features, features.T, precision=lax.Precision.HIGHEST) / EMB
    gram = 0.5 * (gram + gram.T) + jnp.eye(N, dtype=jnp.float32)
    row_blocks = N // (N_PROW * BLOCK)
    col_blocks = N // (N_PCOL * BLOCK)
    gram = gram.reshape(row_blocks, N_PROW, BLOCK, col_blocks, N_PCOL, BLOCK)
    return gram.transpose(1, 0, 2, 4, 3, 5).reshape(N, N)


def setup_inputs(seed: int = 0) -> dict:
    key_of = jax.random.split(jax.random.key(seed), 2)
    blocked = draw_blocked(jax.random.fold_in(key_of[1], 71), 0)
    return dict(blocked=blocked)


def reference(blocked):
    row_blocks = N // (N_PROW * BLOCK)
    col_blocks = N // (N_PCOL * BLOCK)
    matrix = blocked.reshape(N_PROW, row_blocks, BLOCK, N_PCOL, col_blocks, BLOCK)
    matrix = matrix.transpose(1, 0, 2, 4, 3, 5).reshape(N, N)
    width = STEPS * BLOCK
    leading = jnp.tril(jnp.linalg.cholesky(matrix[:width, :width]))
    lower = jax.scipy.linalg.solve_triangular(leading, matrix[width:, :width].T, lower=True).T
    schur = matrix[width:, width:] - jnp.dot(lower, lower.T, precision=lax.Precision.HIGHEST)
    upper_part = jnp.concatenate([leading, jnp.zeros((width, N - width), jnp.float32)], axis=1)
    lower_part = jnp.concatenate([lower, schur], axis=1)
    result = jnp.concatenate([upper_part, lower_part], axis=0)
    result = result.reshape(row_blocks, N_PROW, BLOCK, col_blocks, N_PCOL, BLOCK)
    return result.transpose(1, 0, 2, 4, 3, 5).reshape(N, N)
```

```python
import functools

import jax
import jax.numpy as jnp
from jax import lax
from jax.experimental import pallas as pl
from jax.experimental.pallas import tpu as pltpu
from jax.sharding import PartitionSpec as P

BLOCK = 128
STEPS = 8
WIDTH = BLOCK * STEPS
TILE = 8
TILES = BLOCK // TILE
SIDE = 4
RING = 8
ZCHUNKS = 8
QCHUNKS = 4
ZROWS = WIDTH // ZCHUNKS
QROWS = BLOCK // QCHUNKS

UP = ((0, 1, 2), (1, 2, 3), (2, 3, 4, 5, 6, 7), (3, 4, 5, 6, 7, 0))
DOWN = ((0, 7, 6, 5, 4, 3), (1, 0, 7, 6, 5, 4), (2, 1, 0), (3, 2, 1))


def any_of(value, choices):
    hit = value == choices[0]
    for choice in choices[1:]:
        hit = hit | (value == choice)
    return hit


class Links:
    def __init__(self, ap, aq, wb, zsem, zsend, qsem, qsend, wsem, wsend):
        self.ap, self.aq, self.wb = ap, aq, wb
        self.zsem, self.zsend = zsem, zsend
        self.qsem, self.qsend = qsem, qsend
        self.wsem, self.wsend = wsem, wsend
        self.p, self.q = lax.axis_index("prow"), lax.axis_index("pcol")
        self.y, self.x = self.p // SIDE, self.p % SIDE
        self.z, self.c = self.q // 2, self.q % 2

    def device(self, dx=0, dy=0, dz=0, dc=0):
        prow = (self.y + dy) % SIDE * SIDE + (self.x + dx) % SIDE
        pcol = (self.z + dz) % RING * 2 + (self.c + dc) % 2
        return (prow, pcol)

    def neighbours(self):
        return [
            self.device(dx=1), self.device(dx=-1), self.device(dy=1), self.device(dy=-1),
            self.device(dz=1), self.device(dz=-1), self.device(dc=1),
        ]

    def copy(self, src, dst, send, recv, device):
        return pltpu.make_async_remote_copy(
            src_ref=src, dst_ref=dst, send_sem=send, recv_sem=recv,
            device_id=device, device_id_type=pl.DeviceIdType.MESH,
        )

    def zcopy(self, way, m, t, parity, device):
        j = 2 * m + parity
        part = self.ap.at[j, pl.ds(t * ZROWS, ZROWS)]
        return self.copy(part, part, self.zsend.at[way, m, t], self.zsem.at[j, t], device)

    def zstep(self, m, t):
        here = self.zcopy(0, m, t, self.c, self.device(dz=1))

        @pl.when(self.z != m)
        def _():
            here.wait_recv()

        @pl.when(any_of(self.z, UP[m][:-1]))
        def _():
            here.start()

        @pl.when(any_of(self.z, DOWN[m][:-1]))
        def _():
            self.zcopy(1, m, t, self.c, self.device(dz=-1)).start()

        self.zcopy(2, m, t, self.c, self.device(dc=1)).start()

    def ztwin(self, m, t):
        self.zcopy(2, m, t, 1 - self.c, self.device(dc=1)).wait_recv()

    def zdrain(self):
        for t in range(ZCHUNKS):
            for m in range(4):
                @pl.when(any_of(self.z, UP[m][:-1]))
                def _():
                    self.zcopy(0, m, t, self.c, self.device(dz=1)).wait_send()

                @pl.when(any_of(self.z, DOWN[m][:-1]))
                def _():
                    self.zcopy(1, m, t, self.c, self.device(dz=-1)).wait_send()

                self.zcopy(2, m, t, self.c, self.device(dc=1)).wait_send()

    def qcopy(self, way, i, t):
        device = (self.device(dy=1), self.device(dy=-1), self.device(dx=1), self.device(dx=-1))[way]
        part = self.aq.at[i, pl.ds(t * QROWS, QROWS)]
        return self.copy(part, part, self.qsend.at[way, i, t], self.qsem.at[i, t], device)

    def qways(self, i):
        ys, xs = i // SIDE, i % SIDE
        dx = (self.x - xs + SIDE) % SIDE
        same, own = dx == 0, self.y == ys
        if ys == 0:
            return (same & own, same & (own | (self.y == 3)), (dx == 0) | (dx == 1), dx == 0)
        return (same & (own | (self.y == 2)), same & own, dx == 0, (dx == 0) | (dx == 3))

    def qstep(self, i, t):
        @pl.when(self.p != i)
        def _():
            self.qcopy(0, i, t).wait_recv()

        for way, sends in enumerate(self.qways(i)):
            @pl.when(sends)
            def _():
                self.qcopy(way, i, t).start()

    def qdrain(self):
        for t in range(QCHUNKS):
            for i in range(STEPS):
                for way, sends in enumerate(self.qways(i)):
                    @pl.when(sends)
                    def _():
                        self.qcopy(way, i, t).wait_send()

    def wcopy(self, way, k, j, parity, own=False):
        device = (
            self.device(dy=1), self.device(dy=-1), self.device(dx=1), self.device(dx=-1), self.device(dc=1),
        )[way]
        dst = self.wb.at[k, j]
        src = self.ap.at[j, pl.ds(0, BLOCK)] if own else dst
        return self.copy(src, dst, self.wsend.at[way, k, j // 2], self.wsem.at[k, j], device)

    def wways(self, k):
        ys, xs = k // SIDE, k % SIDE
        dx = (self.x - xs + SIDE) % SIDE
        row = self.y == ys
        if ys == 0:
            return (row, row | (self.y == 3), row & ((dx == 0) | (dx == 1)), row & (dx == 0), self.p != k)
        return (row | (self.y == 2), row, row & (dx == 0), row & ((dx == 0) | (dx == 3)), self.p != k)

    def wstep(self, k, j):
        @pl.when(self.c == j % 2)
        def _():
            @pl.when(self.p != k)
            def _():
                self.wcopy(0, k, j, self.c).wait_recv()

            for way, sends in enumerate(self.wways(k)):
                @pl.when(sends & (self.p != k))
                def _():
                    self.wcopy(way, k, j, self.c).start()
                if way < 4:
                    @pl.when(sends & (self.p == k))
                    def _():
                        self.wcopy(way, k, j, self.c, own=True).start()

    def wtwin(self, k, j):
        @pl.when((self.c != j % 2) & (self.p != k))
        def _():
            self.wcopy(4, k, j, 1 - self.c).wait_recv()

    def wdrain(self):
        for k in range(STEPS):
            for j in range(k, STEPS):
                for way, sends in enumerate(self.wways(k)):
                    @pl.when(sends & (self.c == j % 2))
                    def _():
                        self.wcopy(way, k, j, self.c).wait_send()


def gather_kernel(t_ref, ap_out, aq_out, wb_out, ap, aq, wb, lsem, osem, *sems):
    net = Links(ap, aq, wb, *sems)
    barrier = pltpu.get_barrier_semaphore()
    for device in net.neighbours():
        pl.semaphore_signal(barrier, inc=1, device_id=device, device_id_type=pl.DeviceIdType.MESH)
    head = pltpu.make_async_copy(t_ref.at[pl.ds(0, BLOCK), pl.ds(0, BLOCK)], ap.at[net.q % STEPS, pl.ds(0, BLOCK)], lsem.at[0])
    body = pltpu.make_async_copy(
        t_ref.at[pl.ds(BLOCK, WIDTH - BLOCK), pl.ds(0, BLOCK)],
        ap.at[net.q % STEPS, pl.ds(BLOCK, WIDTH - BLOCK)], lsem.at[1],
    )
    rows = pltpu.make_async_copy(t_ref.at[pl.ds(0, BLOCK)], aq.at[net.p % STEPS], lsem.at[2])

    @pl.when(net.q < STEPS)
    def _():
        head.start()
        body.start()
        head.wait()
        body.wait()

    @pl.when(net.p < STEPS)
    def _():
        rows.start()
        rows.wait()

    pl.semaphore_wait(barrier, 7)
    for m in range(4):
        net.zstep(m, 0)
    for t in range(QCHUNKS):
        for i in range(STEPS):
            @pl.when(net.p == i)
            def _():
                net.qstep(i, t)
    for m in range(4):
        net.ztwin(m, 0)
    for k in range(STEPS):
        @pl.when(net.p == k)
        def _():
            for j in range(STEPS):
                wb[k, j] = ap[j, 0:BLOCK]
    for k in range(STEPS):
        for j in range(k, STEPS):
            net.wstep(k, j)
        if k:
            for m in range(4):
                net.zstep(m, k)
    for t in range(QCHUNKS):
        for i in range(STEPS):
            @pl.when(net.p != i)
            def _():
                net.qstep(i, t)
    for t in range(1, ZCHUNKS):
        for m in range(4):
            net.ztwin(m, t)
    for k in range(STEPS):
        for j in range(k, STEPS):
            net.wtwin(k, j)
    outs = [
        pltpu.make_async_copy(src, dst, osem.at[n])
        for n, (src, dst) in enumerate(((ap, ap_out), (aq, aq_out), (wb, wb_out)))
    ]
    for out in outs:
        out.start()
    net.zdrain()
    net.qdrain()
    net.wdrain()
    for out in outs:
        out.wait()


def row_of(x, j):
    return jnp.broadcast_to(x[j : j + 1, :], (TILE, BLOCK))


def lane_of(x, c):
    return jnp.broadcast_to(x[:, c : c + 1], x.shape)


def times(x, n):
    return x if n == 1 else jnp.concatenate([x] * n, axis=0)


def invert_factor(block):
    sub = lax.broadcasted_iota(jnp.int32, (TILE, BLOCK), 0)
    rows = lax.broadcasted_iota(jnp.int32, (BLOCK, BLOCK), 0)
    lanes = lax.broadcasted_iota(jnp.int32, (BLOCK, BLOCK), 1)
    ident = jnp.where(rows == lanes, 1.0, 0.0).astype(jnp.float32)
    head, rest = block[:TILE], block[TILE:]
    bhead, brest = ident[:TILE], ident[TILE:]
    done = []
    ahead = [lane_of(head, j) for j in range(TILE)]
    for s in range(TILES):
        left = TILES - 1 - s
        first = TILE * s
        col = ahead
        if left:
            below = [lane_of(rest, first + j) for j in range(TILE)]
            ahead = [lane_of(rest[:TILE], first + TILE + j) for j in range(TILE)]
        r, b = head, bhead
        scale, coef = [], {}
        for j in range(TILE):
            scale.append(lax.rsqrt(row_of(col[j], j)))
            line = col[j] * scale[j]
            for k in range(j + 1, TILE):
                coef[j, k] = row_of(line, k)
                col[k] = col[k] - line * coef[j, k]
            ru, bu = row_of(r, j) * scale[j], row_of(b, j) * scale[j]
            if j < TILE - 1:
                low = jnp.where(sub > j, line, 0.0)
                r = jnp.where(sub == j, ru, r - low * ru)
                b = jnp.where(sub == j, bu, b - low * bu)
            else:
                r = jnp.where(sub == j, ru, r)
                b = jnp.where(sub == j, bu, b)
        done.append(b)
        if not left:
            break
        lines = []
        for j in range(TILE):
            line = below[j] * times(scale[j], left)
            lines.append(line)
            for k in range(j + 1, TILE):
                below[k] = below[k] - line * times(coef[j, k], left)
        for m in range(TILE):
            near = lines[m][:TILE]
            for j in range(TILE):
                ahead[j] = ahead[j] - near * row_of(near, j)
        for j in range(TILE):
            rest = rest - lines[j] * times(row_of(r, j), left)
            brest = brest - lines[j] * times(row_of(b, j), left)
        head, rest = rest[:TILE], rest[TILE:]
        bhead, brest = brest[:TILE], brest[TILE:]
    return jnp.concatenate(done, axis=0)


def split(x):
    high = x.astype(jnp.bfloat16)
    return high, (x - high.astype(jnp.float32)).astype(jnp.bfloat16)


NN = (((1,), (0,)), ((), ()))
TN = (((0,), (0,)), ((), ()))
NT = (((1,), (1,)), ((), ()))


def dot3(a, b, dims):
    one = functools.partial(lax.dot_general, dimension_numbers=dims, preferred_element_type=jnp.float32)
    return one(a[0], b[0]) + one(a[0], b[1]) + one(a[1], b[0])


def update_kernel(t_ref, ap, aq, wb, out, lpf, uh, ul, xh, xl, aph, apl, aqh, aql, diag):
    p, q = lax.axis_index("prow"), lax.axis_index("pcol")
    xh[...] = jnp.zeros_like(xh)
    xl[...] = jnp.zeros_like(xl)
    for j in range(STEPS):
        aqh[j * BLOCK : (j + 1) * BLOCK, :], aql[j * BLOCK : (j + 1) * BLOCK, :] = split(aq[j])
        aph[:, j * BLOCK : (j + 1) * BLOCK], apl[:, j * BLOCK : (j + 1) * BLOCK] = split(ap[j])
    diag[...] = wb[0, 0]

    def step(k, carry):
        inv = invert_factor(diag[...])
        ih, il = split(inv)
        for kk in range(STEPS):
            lo, hi = kk * BLOCK, (kk + 1) * BLOCK

            @pl.when(k == kk)
            def _():
                xh[lo:hi, lo:hi] = ih
                xl[lo:hi, lo:hi] = il
                if kk:
                    lead = (uh[:lo, lo:hi], ul[:lo, lo:hi])
                    gx = split(dot3(lead, (xh[:lo, :lo], xl[:lo, :lo]), TN))
                    xrow = split(-dot3((ih, il), gx, NN))
                    xh[lo:hi, :lo], xl[lo:hi, :lo] = xrow
                if kk < STEPS - 1:
                    g = jnp.concatenate([wb[kk, j] for j in range(kk + 1, STEPS)], axis=1)
                    if kk:
                        g = g - dot3(lead, (uh[:lo, hi:], ul[:lo, hi:]), TN)
                    urow = split(dot3((ih, il), split(g), NN))
                    uh[lo:hi, hi:], ul[lo:hi, hi:] = urow
                    nxt = (uh[:hi, hi : hi + BLOCK], ul[:hi, hi : hi + BLOCK])
                    diag[...] = wb[kk + 1, kk + 1] - dot3(nxt, nxt, TN)

        return carry

    lax.fori_loop(0, STEPS, step, 0)
    lqh, lql = uh, ul
    wide = 2 * BLOCK
    for b in range(STEPS // 2):
        end = wide * (b + 1)
        rows = pl.ds(wide * b, wide)
        xb = (xh[rows, :end], xl[rows, :end])
        lqh[rows, :], lql[rows, :] = split(dot3(xb, (aqh[:end, :], aql[:end, :]), NN))

        def part(i, carry, b=b, end=end, xb=xb, rows=rows):
            mine = pl.ds(pl.multiple_of(i * wide, wide), wide)
            lp = dot3((aph[mine, :end], apl[mine, :end]), xb, NT)
            lpf[2 * b, mine] = lp[:, :BLOCK]
            lpf[2 * b + 1, mine] = lp[:, BLOCK:]
            prev = t_ref[mine, :] if b == 0 else out[mine, :]
            out[mine, :] = prev - dot3(split(lp), (lqh[rows, :], lql[rows, :]), NN)
            return carry

        lax.fori_loop(0, WIDTH // wide, part, 0)

    @pl.when(p < STEPS)
    def _():
        out[0:BLOCK, :] = jnp.zeros((BLOCK, WIDTH), jnp.float32)

    @pl.when(q < STEPS)
    def _():
        out[BLOCK:, 0:BLOCK] = lpf[q % STEPS, BLOCK:]
        top = lpf[q % STEPS, 0:BLOCK]
        rows = lax.broadcasted_iota(jnp.int32, (BLOCK, BLOCK), 0) + p * BLOCK
        lanes = lax.broadcasted_iota(jnp.int32, (BLOCK, BLOCK), 1) + q * BLOCK
        out[0:BLOCK, 0:BLOCK] = jnp.where((p >= STEPS) | (rows >= lanes), top, 0.0)


def per_device(blocked):
    f32, bf16 = jnp.float32, jnp.bfloat16
    hbm = pl.BlockSpec(memory_space=pl.ANY)
    slabs = [(STEPS, WIDTH, BLOCK), (STEPS, BLOCK, WIDTH), (STEPS, STEPS, BLOCK, BLOCK)]
    dma = pltpu.SemaphoreType.DMA
    ap, aq, wb = pl.pallas_call(
        gather_kernel,
        name="gather",
        out_shape=[jax.ShapeDtypeStruct(s, f32) for s in slabs],
        in_specs=[hbm],
        out_specs=[hbm] * 3,
        scratch_shapes=[
            *(pltpu.VMEM(s, f32) for s in slabs),
            dma((3,)), dma((3,)),
            dma((8, ZCHUNKS)), dma((3, 4, ZCHUNKS)),
            dma((8, QCHUNKS)), dma((4, 8, QCHUNKS)),
            dma((8, 8)), dma((5, 8, 4)),
        ],
        compiler_params=pltpu.CompilerParams(collective_id=0, has_side_effects=True, vmem_limit_bytes=40 << 20),
    )(blocked)
    vmem = pl.BlockSpec(memory_space=pltpu.VMEM)
    square = (WIDTH, WIDTH)
    return pl.pallas_call(
        update_kernel,
        name="update",
        out_shape=jax.ShapeDtypeStruct(square, f32),
        in_specs=[vmem] * 4,
        out_specs=vmem,
        scratch_shapes=[
            pltpu.VMEM(slabs[0], f32),
            *(pltpu.VMEM(square, bf16) for _ in range(8)),
            pltpu.VMEM((BLOCK, BLOCK), f32),
        ],
        compiler_params=pltpu.CompilerParams(vmem_limit_bytes=60 << 20),
    )(blocked, ap, aq, wb)


def solution(mesh):
    return jax.shard_map(
        per_device,
        mesh=mesh,
        in_specs=(P("prow", "pcol"),),
        out_specs=P("prow", "pcol"),
        check_vma=False,
    )
```

```python
import functools

import jax
import jax.numpy as jnp
from jax import lax
from jax.experimental import pallas as pl
from jax.experimental.pallas import tpu as pltpu
from jax.sharding import PartitionSpec as P

BLOCK = 128
STEPS = 8
WIDTH = BLOCK * STEPS
TILE = 8
TILES = BLOCK // TILE
SIDE = 4
RING = 8
CHUNKS = 8
WIDE = 2 * BLOCK
ROUNDS = WIDTH // WIDE

UP_FIRST = ((0, 1, 2, 3, 4), (1, 2, 3, 4), (2, 3, 4, 5, 6), (3, 4, 5, 6, 7))
DOWN_FIRST = ((0, 7, 6, 5), (1, 0, 7, 6, 5), (2, 1, 0, 7), (3, 2, 1, 0))
UP = ((0, 1, 2), (1, 2, 3), (2, 3, 4, 5, 6, 7), (3, 4, 5, 6, 7, 0))
DOWN = ((0, 7, 6, 5, 4, 3), (1, 0, 7, 6, 5, 4), (2, 1, 0), (3, 2, 1))


def any_of(value, choices):
    hit = value == choices[0]
    for choice in choices[1:]:
        hit = hit | (value == choice)
    return hit


def table(value, entries):
    out = jnp.int32(entries[0])
    for n, entry in enumerate(entries[1:], 1):
        out = jnp.where(value == n, jnp.int32(entry), out)
    return out


def hops(ups, downs, m):
    return [ups[m].index(z) if z in ups[m] else downs[m].index(z) for z in range(RING)]


class Links:
    def __init__(self, ap, aq, wb, zsem, zsend, qsem, qsend, wsem, wsend):
        self.ap, self.aq, self.wb = ap, aq, wb
        self.zsem, self.zsend = zsem, zsend
        self.qsem, self.qsend = qsem, qsend
        self.wsem, self.wsend = wsem, wsend
        self.p, self.q = lax.axis_index("prow"), lax.axis_index("pcol")
        self.y, self.x = self.p // SIDE, self.p % SIDE
        self.z, self.c = self.q // 2, self.q % 2
        self.zhops = [table(self.z, hops(UP, DOWN, m)) for m in range(4)]
        self.zfirst = [table(self.z, hops(UP_FIRST, DOWN_FIRST, m)) for m in range(4)]
        self.up = [any_of(self.z, UP[m][:-1]) for m in range(4)]
        self.down = [any_of(self.z, DOWN[m][:-1]) for m in range(4)]
        self.up_first = [any_of(self.z, UP_FIRST[m][:-1]) for m in range(4)]
        self.down_first = [any_of(self.z, DOWN_FIRST[m][:-1]) for m in range(4)]
        self.qhops, self.qways = [], []
        for i in range(STEPS):
            ys, dx = i // SIDE, (self.x - i % SIDE + SIDE) % SIDE
            own, same = self.y == ys, dx == 0
            self.qhops.append(table(self.y, (0, 1, 2, 1) if ys == 0 else (1, 0, 1, 2)) + table(dx, (0, 1, 2, 1)))
            if ys == 0:
                ways = (same & own, same & (own | (self.y == 3)), same | (dx == 1), same)
            else:
                ways = (same & (own | (self.y == 2)), same & own, same, same | (dx == 3))
            self.qways.append(ways)

    def device(self, dx=0, dy=0, dz=0, dc=0):
        prow = (self.y + dy) % SIDE * SIDE + (self.x + dx) % SIDE
        pcol = (self.z + dz) % RING * 2 + (self.c + dc) % 2
        return (prow, pcol)

    def neighbours(self):
        around = [self.device(dx=n) for n in (1, 2, 3)] + [self.device(dy=n) for n in (1, 2, 3)]
        return around + [self.device(dz=1), self.device(dz=RING - 1), self.device(dc=1)]

    def copy(self, src, dst, send, recv, device):
        return pltpu.make_async_remote_copy(
            src_ref=src, dst_ref=dst, send_sem=send, recv_sem=recv,
            device_id=device, device_id_type=pl.DeviceIdType.MESH,
        )

    def zcopy(self, way, m, t, parity, first=False):
        j = 2 * m + parity
        device = (self.device(dz=1), self.device(dz=RING - 1), self.device(dc=1))[way]
        part = self.ap.at[j, pl.ds(0 if first else pl.multiple_of(t * BLOCK, BLOCK), BLOCK)]
        return self.copy(part, part, self.zsend.at[int(first), way, m], self.zsem.at[j, t], device)

    def zitem(self, m, t, first=False):
        up, down = (self.up_first, self.down_first) if first else (self.up, self.down)

        @pl.when(self.z != m)
        def _():
            self.zcopy(0, m, t, self.c, first).wait_recv()

        for way, sends in enumerate((up[m], down[m])):
            @pl.when(sends)
            def _():
                self.zcopy(way, m, t, self.c, first).start()

        self.zcopy(2, m, t, self.c, first).start()

    def zslot(self, slot):
        for m in range(4):
            t = slot - self.zhops[m]

            @pl.when((t >= 1) & (t < CHUNKS))
            def _():
                self.zitem(m, t)

    def ztwin(self, m, t, first=False):
        self.zcopy(2, m, t, 1 - self.c, first).wait_recv()

    def qcopy(self, way, i, t):
        device = (self.device(dy=1), self.device(dy=3), self.device(dx=1), self.device(dx=3))[way]
        part = self.aq.at[i, t]
        return self.copy(part, part, self.qsend.at[way, i], self.qsem.at[i, t], device)

    def qslot(self, slot):
        for i in range(STEPS):
            t = slot - self.qhops[i]

            @pl.when((t >= 0) & (t < CHUNKS))
            def _():
                @pl.when(self.p != i)
                def _():
                    self.qcopy(0, i, t).wait_recv()

                for way, sends in enumerate(self.qways[i]):
                    @pl.when(sends)
                    def _():
                        self.qcopy(way, i, t).start()

    def wcopy(self, way, k, m, parity, own=False):
        step = way % 3 + 1
        device = self.device(dc=1) if way == 6 else self.device(dy=step) if way >= 3 else self.device(dx=step)
        j = 2 * m + parity
        dst = self.wb.at[k, j]
        src = self.ap.at[j, pl.ds(0, BLOCK)] if own else dst
        return self.copy(src, dst, self.wsend.at[way, k], self.wsem.at[k, j], device)

    def wsource(self, k):
        @pl.when(self.p == k)
        def _():
            for m in range(k // 2, STEPS // 2):
                for way in range(6):
                    self.wcopy(way, k, m, self.c, own=True).start()

    def wrow(self, k):
        @pl.when((self.y == k // SIDE) & (self.p != k))
        def _():
            for m in range(k // 2, STEPS // 2):
                self.wcopy(0, k, m, self.c).wait_recv()
                for way in (3, 4, 5, 6):
                    self.wcopy(way, k, m, self.c).start()

    def wrest(self, k):
        @pl.when(self.y != k // SIDE)
        def _():
            def item(m, carry):
                self.wcopy(0, k, m, self.c).wait_recv()
                self.wcopy(6, k, m, self.c).start()
                return carry

            lax.fori_loop(k // 2, STEPS // 2, item, 0)

    def wtwin(self, k):
        @pl.when(self.p != k)
        def _():
            def item(m, carry):
                self.wcopy(6, k, m, 1 - self.c).wait_recv()
                return carry

            lax.fori_loop(k // 2, STEPS // 2, item, 0)

    def drain(self):
        for m in range(4):
            for way, first, later in (
                (0, self.up_first[m], self.up[m]), (1, self.down_first[m], self.down[m]), (2, None, None),
            ):
                device = self.device(dc=1)
                one, rest = self.ap.at[0, pl.ds(0, BLOCK)], self.ap.at[0, pl.ds(0, WIDTH - BLOCK)]
                head = self.copy(one, one, self.zsend.at[1, way, m], self.zsem.at[0, 0], device)
                tail = self.copy(rest, rest, self.zsend.at[0, way, m], self.zsem.at[0, 0], device)
                if first is None:
                    head.wait_send()
                    tail.wait_send()
                else:
                    pl.when(first)(head.wait_send)
                    pl.when(later)(tail.wait_send)
        for i in range(STEPS):
            for way, sends in enumerate(self.qways[i]):
                whole = self.copy(
                    self.aq.at[i], self.aq.at[i], self.qsend.at[way, i], self.qsem.at[0, 0], self.device(dc=1)
                )
                pl.when(sends)(whole.wait_send)
        for k in range(STEPS):
            part = self.wb.at[k, pl.ds(0, STEPS // 2 - k // 2)]
            for way in range(7):
                sends = (self.p == k) if way < 3 else (self.y == k // SIDE) if way < 6 else (self.p != k)
                whole = self.copy(part, part, self.wsend.at[way, k], self.wsem.at[0, 0], self.device(dc=1))
                pl.when(sends)(whole.wait_send)


def row_of(x, j):
    return jnp.broadcast_to(x[j : j + 1, :], (TILE, BLOCK))


def lane_of(x, c):
    return jnp.broadcast_to(x[:, c : c + 1], x.shape)


def times(x, n):
    return x if n == 1 else jnp.concatenate([x] * n, axis=0)


def invert_factor(block):
    sub = lax.broadcasted_iota(jnp.int32, (TILE, BLOCK), 0)
    rows = lax.broadcasted_iota(jnp.int32, (BLOCK, BLOCK), 0)
    lanes = lax.broadcasted_iota(jnp.int32, (BLOCK, BLOCK), 1)
    ident = jnp.where(rows == lanes, 1.0, 0.0).astype(jnp.float32)
    head, rest = block[:TILE], block[TILE:]
    bhead, brest = ident[:TILE], ident[TILE:]
    done = []
    ahead = [lane_of(head, j) for j in range(TILE)]
    for s in range(TILES):
        left = TILES - 1 - s
        first = TILE * s
        col = ahead
        if left:
            below = [lane_of(rest, first + j) for j in range(TILE)]
            ahead = [lane_of(rest[:TILE], first + TILE + j) for j in range(TILE)]
        r, b = head, bhead
        scale, coef = [], {}
        for j in range(TILE):
            scale.append(lax.rsqrt(row_of(col[j], j)))
            line = col[j] * scale[j]
            for k in range(j + 1, TILE):
                coef[j, k] = row_of(line, k)
                col[k] = col[k] - line * coef[j, k]
            ru, bu = row_of(r, j) * scale[j], row_of(b, j) * scale[j]
            if j < TILE - 1:
                low = jnp.where(sub > j, line, 0.0)
                r = jnp.where(sub == j, ru, r - low * ru)
                b = jnp.where(sub == j, bu, b - low * bu)
            else:
                r = jnp.where(sub == j, ru, r)
                b = jnp.where(sub == j, bu, b)
        done.append(b)
        if not left:
            break
        lines = []
        for j in range(TILE):
            line = below[j] * times(scale[j], left)
            lines.append(line)
            for k in range(j + 1, TILE):
                below[k] = below[k] - line * times(coef[j, k], left)
        for m in range(TILE):
            near = lines[m][:TILE]
            for j in range(TILE):
                ahead[j] = ahead[j] - near * row_of(near, j)
        for j in range(TILE):
            rest = rest - lines[j] * times(row_of(r, j), left)
            brest = brest - lines[j] * times(row_of(b, j), left)
        head, rest = rest[:TILE], rest[TILE:]
        bhead, brest = brest[:TILE], brest[TILE:]
    return jnp.concatenate(done, axis=0)


def split(x):
    high = x.astype(jnp.bfloat16)
    return high, (x - high.astype(jnp.float32)).astype(jnp.bfloat16)


NN = (((1,), (0,)), ((), ()))
TN = (((0,), (0,)), ((), ()))
NT = (((1,), (1,)), ((), ()))


def dot3(a, b, dims):
    one = functools.partial(lax.dot_general, dimension_numbers=dims, preferred_element_type=jnp.float32)
    return one(a[0], b[0]) + one(a[0], b[1]) + one(a[1], b[0])


def kernel(t_ref, out, ap, aq, wb, tv, lpf, uh, ul, xh, xl, lph, lpl, lqh, lql, diag, lsem, osem, *sems):
    net = Links(ap, aq, wb, *sems)
    p, q = net.p, net.q
    barrier = pltpu.get_barrier_semaphore()
    for device in net.neighbours():
        pl.semaphore_signal(barrier, inc=1, device_id=device, device_id_type=pl.DeviceIdType.MESH)
    cols = pl.ds(0, BLOCK)
    head = pltpu.make_async_copy(t_ref.at[cols, cols], ap.at[q % STEPS, cols], lsem.at[0])
    later = pl.ds(BLOCK, WIDTH - BLOCK)
    body = pltpu.make_async_copy(t_ref.at[later, cols], ap.at[q % STEPS, later], lsem.at[1])
    rows = [
        pltpu.make_async_copy(t_ref.at[cols, pl.ds(t * BLOCK, BLOCK)], aq.at[p % STEPS, t], lsem.at[2 + t])
        for t in range(CHUNKS)
    ]
    whole = pltpu.make_async_copy(t_ref, tv, lsem.at[2 + CHUNKS])

    @pl.when(q < STEPS)
    def _():
        head.start()
        body.start()

    @pl.when(p < STEPS)
    def _():
        for row in rows:
            row.start()

    whole.start()
    pl.semaphore_wait(barrier, 9)

    @pl.when(q < STEPS)
    def _():
        head.wait()
        body.wait()

    @pl.when(p < STEPS)
    def _():
        for row in rows:
            row.wait()

    for slot in range(5):
        for m in range(4):
            @pl.when(net.zfirst[m] == slot)
            def _():
                net.zitem(m, 0, first=True)
    for k in range(STEPS):
        net.wsource(k)
    for m in range(4):
        net.ztwin(m, 0, first=True)
    for k in range(STEPS):
        @pl.when(p == k)
        def _():
            for j in range(STEPS):
                wb[k, j] = ap[j, 0:BLOCK]
    for k in range(STEPS):
        net.wrow(k)
    xh[...] = jnp.zeros_like(xh)
    xl[...] = jnp.zeros_like(xl)
    net.wrest(0)
    net.wtwin(0)
    diag[...] = wb[0, 0]

    def step(k, carry):
        net.zslot(k + 1)
        net.qslot(k)

        @pl.when(k < STEPS - 1)
        def _():
            net.wrest(k + 1)

        inv = invert_factor(diag[...])

        @pl.when(k < STEPS - 1)
        def _():
            net.wtwin(k + 1)

        ih, il = split(inv)
        for kk in range(STEPS):
            lo, hi = kk * BLOCK, (kk + 1) * BLOCK

            @pl.when(k == kk)
            def _():
                xh[lo:hi, lo:hi] = ih
                xl[lo:hi, lo:hi] = il
                if kk:
                    lead = (uh[:lo, lo:hi], ul[:lo, lo:hi])
                    gx = split(dot3(lead, (xh[:lo, :lo], xl[:lo, :lo]), TN))
                    xrow = split(-dot3((ih, il), gx, NN))
                    xh[lo:hi, :lo], xl[lo:hi, :lo] = xrow
                if kk < STEPS - 1:
                    g = jnp.concatenate([wb[kk, j] for j in range(kk + 1, STEPS)], axis=1)
                    if kk:
                        g = g - dot3(lead, (uh[:lo, hi:], ul[:lo, hi:]), TN)
                    urow = split(dot3((ih, il), split(g), NN))
                    uh[lo:hi, hi:], ul[lo:hi, hi:] = urow
                    nxt = (uh[:hi, hi : hi + BLOCK], ul[:hi, hi : hi + BLOCK])
                    diag[...] = wb[kk + 1, kk + 1] - dot3(nxt, nxt, TN)

        return carry

    lax.fori_loop(0, STEPS, step, 0)
    whole.wait()

    def spread(u, carry):
        net.zslot(9 + 2 * u)
        net.qslot(8 + 2 * u)
        net.zslot(10 + 2 * u)
        net.qslot(9 + 2 * u)
        for m in range(4):
            pl.when(u > 0)(lambda: net.ztwin(m, 2 * u))
            net.ztwin(m, 2 * u + 1)
        mine = pl.ds(pl.multiple_of(u * WIDE, WIDE), WIDE)
        apu = split(jnp.concatenate([ap[j, mine] for j in range(STEPS)], axis=1))
        aqu = split(jnp.concatenate(
            [jnp.concatenate([aq[i, 2 * u], aq[i, 2 * u + 1]], axis=1) for i in range(STEPS)], axis=0))
        for b in range(ROUNDS):
            lo, hi = b * WIDE, (b + 1) * WIDE
            xb = (xh[lo:hi, :hi], xl[lo:hi, :hi])
            lp = dot3((apu[0][:, :hi], apu[1][:, :hi]), xb, NT)
            lpf[2 * b, mine] = lp[:, :BLOCK]
            lpf[2 * b + 1, mine] = lp[:, BLOCK:]
            lph[u, :, lo:hi], lpl[u, :, lo:hi] = split(lp)
            lqh[u, lo:hi, :], lql[u, lo:hi, :] = split(dot3(xb, (aqu[0][:hi], aqu[1][:hi]), NN))

        def cell(a, b):
            where = (pl.ds(pl.multiple_of(a * WIDE, WIDE), WIDE), pl.ds(pl.multiple_of(b * WIDE, WIDE), WIDE))
            tv[where] = tv[where] - dot3((lph[a], lpl[a]), (lqh[b], lql[b]), NN)

        def cells(v, carry):
            cell(u, v)
            cell(v, u)
            return carry

        lax.fori_loop(0, u, cells, 0)
        cell(u, u)
        return carry

    lax.fori_loop(0, ROUNDS, spread, 0)

    @pl.when(p < STEPS)
    def _():
        tv[0:BLOCK, :] = jnp.zeros((BLOCK, WIDTH), jnp.float32)

    @pl.when(q < STEPS)
    def _():
        tv[BLOCK:, 0:BLOCK] = lpf[q % STEPS, BLOCK:]
        top = lpf[q % STEPS, 0:BLOCK]
        down = lax.broadcasted_iota(jnp.int32, (BLOCK, BLOCK), 0) + p * BLOCK
        across = lax.broadcasted_iota(jnp.int32, (BLOCK, BLOCK), 1) + q * BLOCK
        tv[0:BLOCK, 0:BLOCK] = jnp.where((p >= STEPS) | (down >= across), top, 0.0)

    result = pltpu.make_async_copy(tv, out, osem)
    result.start()
    net.drain()
    result.wait()


def per_device(blocked):
    f32, bf16 = jnp.float32, jnp.bfloat16
    hbm = pl.BlockSpec(memory_space=pl.ANY)
    dma, square = pltpu.SemaphoreType.DMA, (WIDTH, WIDTH)
    return pl.pallas_call(
        kernel,
        name="factor",
        out_shape=jax.ShapeDtypeStruct(square, f32),
        in_specs=[hbm],
        out_specs=hbm,
        scratch_shapes=[
            pltpu.VMEM((STEPS, WIDTH, BLOCK), f32),
            pltpu.VMEM((STEPS, CHUNKS, BLOCK, BLOCK), f32),
            pltpu.VMEM((STEPS, STEPS, BLOCK, BLOCK), f32),
            pltpu.VMEM(square, f32),
            pltpu.VMEM((STEPS, WIDTH, BLOCK), f32),
            *(pltpu.VMEM(square, bf16) for _ in range(4)),
            *(pltpu.VMEM((ROUNDS, WIDE, WIDTH), bf16) for _ in range(2)),
            *(pltpu.VMEM((ROUNDS, WIDTH, WIDE), bf16) for _ in range(2)),
            pltpu.VMEM((BLOCK, BLOCK), f32),
            dma((3 + CHUNKS,)), dma,
            dma((STEPS, CHUNKS)), dma((2, 3, 4)),
            dma((STEPS, CHUNKS)), dma((4, STEPS)),
            dma((STEPS, STEPS)), dma((7, STEPS)),
        ],
        compiler_params=pltpu.CompilerParams(collective_id=0, has_side_effects=True, vmem_limit_bytes=58 << 20),
    )(blocked)


def solution(mesh):
    return jax.shard_map(
        per_device,
        mesh=mesh,
        in_specs=(P("prow", "pcol"),),
        out_specs=P("prow", "pcol"),
        check_vma=False,
    )
```

```python
import functools

import jax
import jax.numpy as jnp
from jax import lax
from jax.experimental import pallas as pl
from jax.experimental.pallas import tpu as pltpu
from jax.sharding import PartitionSpec as P

BLOCK = 128
STEPS = 8
WIDTH = BLOCK * STEPS
TILE = 8
TILES = BLOCK // TILE
SIDE = 4
RING = 8
CHUNKS = 8
STAGGER = 1
BEFORE = 5
EXTRA = 2
START = 3
AFTER = 0
PASS = (1, 2, 4)
WIDE = 2 * BLOCK
ROUNDS = WIDTH // WIDE

UP_FIRST = ((0, 1, 2, 3, 4), (1, 2, 3, 4), (2, 3, 4, 5, 6), (3, 4, 5, 6, 7))
DOWN_FIRST = ((0, 7, 6, 5), (1, 0, 7, 6, 5), (2, 1, 0, 7), (3, 2, 1, 0))
UP = ((0, 1, 2), (1, 2, 3), (2, 3, 4, 5, 6, 7), (3, 4, 5, 6, 7, 0))
DOWN = ((0, 7, 6, 5, 4, 3), (1, 0, 7, 6, 5, 4), (2, 1, 0), (3, 2, 1))


def any_of(value, choices):
    hit = value == choices[0]
    for choice in choices[1:]:
        hit = hit | (value == choice)
    return hit


def table(value, entries):
    out = jnp.int32(entries[0])
    for n, entry in enumerate(entries[1:], 1):
        out = jnp.where(value == n, jnp.int32(entry), out)
    return out


def hops(ups, downs, m):
    return [ups[m].index(z) if z in ups[m] else downs[m].index(z) for z in range(RING)]


class Links:
    def __init__(self, ap, aq, wb, zsem, zsend, qsem, qsend, wsem, wsend, fsend):
        self.ap, self.aq, self.wb = ap, aq, wb
        self.zsem, self.zsend = zsem, zsend
        self.qsem, self.qsend = qsem, qsend
        self.wsem, self.wsend, self.fsend = wsem, wsend, fsend
        self.p, self.q = lax.axis_index("prow"), lax.axis_index("pcol")
        self.y, self.x = self.p // SIDE, self.p % SIDE
        self.z, self.c = self.q // 2, self.q % 2
        self.zhops = [table(self.z, hops(UP, DOWN, m)) for m in range(4)]
        self.zfirst = [table(self.z, hops(UP_FIRST, DOWN_FIRST, m)) for m in range(4)]
        self.up = [any_of(self.z, UP[m][:-1]) for m in range(4)]
        self.down = [any_of(self.z, DOWN[m][:-1]) for m in range(4)]
        self.up_first = [any_of(self.z, UP_FIRST[m][:-1]) for m in range(4)]
        self.down_first = [any_of(self.z, DOWN_FIRST[m][:-1]) for m in range(4)]
        self.beside = (self.device(dy=1), self.device(dy=3), self.device(dx=1), self.device(dx=3))
        self.along = (self.device(dz=1), self.device(dz=RING - 1), self.device(dc=1))
        self.qhops, self.ways = [], []
        for i in range(STEPS):
            ys, dx = i // SIDE, (self.x - i % SIDE + SIDE) % SIDE
            row, same = self.y == ys, dx == 0
            self.qhops.append(table(self.y, (0, 1, 2, 1) if ys == 0 else (1, 0, 1, 2)) + table(dx, (0, 1, 2, 1)))
            turn = row | (self.y == (3 if ys == 0 else 2))
            on = same | (dx == (1 if ys == 0 else 3))
            ways = []
            for down, across in ((same, True), (True, row)):
                one, two = (row & down, turn & down), (on & across, same & across)
                ways.append((*(one if ys == 0 else one[::-1]), *(two if ys == 0 else two[::-1])))
            self.ways.append(ways)

    def device(self, dx=0, dy=0, dz=0, dc=0):
        prow = (self.y + dy) % SIDE * SIDE + (self.x + dx) % SIDE
        pcol = (self.z + dz) % RING * 2 + (self.c + dc) % 2
        return (prow, pcol)

    def neighbours(self):
        around = [self.device(dx=n) for n in (1, 2, 3)] + [self.device(dy=n) for n in (1, 2, 3)]
        return around + [self.device(dz=n) for n in range(1, RING)] + [self.device(dc=1)]

    def copy(self, src, dst, send, recv, device):
        return pltpu.make_async_remote_copy(
            src_ref=src, dst_ref=dst, send_sem=send, recv_sem=recv,
            device_id=device, device_id_type=pl.DeviceIdType.MESH,
        )

    def zcopy(self, way, m, t, parity, first=False):
        j = 2 * m + parity
        part = self.ap.at[j, pl.ds(0 if first else pl.multiple_of(t * BLOCK, BLOCK), BLOCK)]
        return self.copy(part, part, self.zsend.at[int(first), way, m], self.zsem.at[j, t], self.along[way])

    def zitem(self, m, t, first=False):
        up, down = (self.up_first, self.down_first) if first else (self.up, self.down)

        @pl.when(self.z != m)
        def _():
            self.zcopy(0, m, t, self.c, first).wait_recv()

        for way, sends in enumerate((up[m], down[m])):
            @pl.when(sends)
            def _():
                self.zcopy(way, m, t, self.c, first).start()

        self.zcopy(2, m, t, self.c, first).start()

    def zslot(self, slot):
        for m in range(4):
            t = slot - self.zhops[m]

            @pl.when((t >= 1) & (t < CHUNKS))
            def _():
                self.zitem(m, t)

    def ztwin(self, m, t, first=False):
        self.zcopy(2, m, t, 1 - self.c, first).wait_recv()

    def qcopy(self, way, i, t, order=0):
        part = self.aq.at[i, t]
        return self.copy(part, part, self.qsend.at[order, way, i], self.qsem.at[i, t], self.beside[way])

    def qslot(self, slot):
        for i in range(STEPS):
            t = slot - self.qhops[i]

            @pl.when((t >= 0) & (t < CHUNKS))
            def _():
                @pl.when(self.p != i)
                def _():
                    self.qcopy(0, i, t).wait_recv()

                odd = t % 2
                for way, (even_sends, odd_sends) in enumerate(zip(*self.ways[i])):
                    @pl.when(jnp.where(odd == 1, odd_sends, even_sends))
                    def _():
                        self.qcopy(way, i, t, odd).start()

    def wcopy(self, way, k, m, parity, own=False):
        device = self.along[2] if way == 4 else self.beside[way]
        j = 2 * m + parity
        dst = self.wb.at[k, j]
        src = self.ap.at[j, pl.ds(0, BLOCK)] if own else dst
        send = self.wsend.at[way, m * (m + 1) - 2 + k]
        return self.copy(src, dst, send, self.wsem.at[k, j], device)

    def wneeded(self, k, m):
        return self.c == 1 if k == 2 * m + 1 else self.c >= 0

    def wslot(self, slot):
        for m in range(1, 4):
            for k in range(2 * m + 2):
                @pl.when((self.zfirst[m] + self.qhops[k] + STAGGER * (m - 1) == slot) & self.wneeded(k, m))
                def _():
                    @pl.when(self.p == k)
                    def _():
                        for way in range(4):
                            pl.when(self.ways[k][0][way])(self.wcopy(way, k, m, self.c, own=True).start)

                    @pl.when(self.p != k)
                    def _():
                        self.wcopy(0, k, m, self.c).wait_recv()
                        for way in range(4):
                            pl.when(self.ways[k][0][way])(self.wcopy(way, k, m, self.c).start)
                        self.wcopy(4, k, m, self.c).start()

    def fcopy(self, n, k, parity, own=False):
        if n < 7:
            device = self.device(dz=(4, 3, 5, 2, 6, 1, 7)[n])
        elif n < 13:
            step = (2, 1, 3)[(n - 7) % 3]
            device = self.device(dy=step) if n < 10 else self.device(dx=step)
        else:
            device = self.along[2]
        dst = self.wb.at[k, parity]
        src = self.ap.at[parity, pl.ds(0, BLOCK)] if own else dst
        return self.copy(src, dst, self.fsend.at[n, k], self.wsem.at[k, parity], device)

    def fsource(self):
        for k in range(2):
            @pl.when((self.p == k) & (self.z == 0) & (k <= self.c))
            def _():
                for n in range(14):
                    self.fcopy(n, k, self.c, own=True).start()

    def fpass(self, stage):
        for k in range(2):
            needed = k <= self.c
            if stage == 0:
                here, sends = (self.p == k) & (self.z != 0), range(7, 14)
            elif stage == 1:
                here, sends = (self.x == k) & (self.y != 0), range(10, 14)
            else:
                here, sends = self.x != k, range(13, 14)

            @pl.when(here & needed)
            def _():
                self.fcopy(0, k, self.c).wait_recv()
                for n in sends:
                    self.fcopy(n, k, self.c).start()

    def wtwin(self, j):
        @pl.when(self.c != j % 2)
        def _():
            def item(k, carry):
                part = self.wb.at[k, j]
                twin = self.copy(part, part, self.fsend.at[0, 0], self.wsem.at[k, j], self.along[2])
                pl.when((j < 2) | (self.p != k))(twin.wait_recv)
                return carry

            lax.fori_loop(0, j + 1, item, 0)

    def drain(self):
        for m in range(4):
            for way, first, later in (
                (0, self.up_first[m], self.up[m]), (1, self.down_first[m], self.down[m]), (2, None, None),
            ):
                device = self.device(dc=1)
                one, rest = self.ap.at[0, pl.ds(0, BLOCK)], self.ap.at[0, pl.ds(0, WIDTH - BLOCK)]
                head = self.copy(one, one, self.zsend.at[1, way, m], self.zsem.at[0, 0], device)
                tail = self.copy(rest, rest, self.zsend.at[0, way, m], self.zsem.at[0, 0], device)
                if first is None:
                    head.wait_send()
                    tail.wait_send()
                else:
                    pl.when(first)(head.wait_send)
                    pl.when(later)(tail.wait_send)
        for i in range(STEPS):
            half = self.aq.at[i, pl.ds(0, CHUNKS // 2)]
            for order in range(2):
                for way, sends in enumerate(self.ways[i][order]):
                    every = self.copy(half, half, self.qsend.at[order, way, i], self.qsem.at[0, 0], self.beside[way])
                    pl.when(sends)(every.wait_send)
        for m in range(1, 4):
            for k in range(2 * m + 2):
                for way in range(5):
                    sends = self.ways[k][0][way] if way < 4 else self.p != k
                    pl.when(sends & self.wneeded(k, m))(self.wcopy(way, k, m, self.c).wait_send)
        for k in range(2):
            for n in range(14):
                line = (self.p == k) & (self.z == 0) if n < 7 else self.p == k if n < 10 else self.x == k if n < 13 else True
                pl.when(line & (k <= self.c))(self.fcopy(n, k, self.c).wait_send)


def row_of(x, j):
    return jnp.broadcast_to(x[j : j + 1, :], (TILE, BLOCK))


def lane_of(x, c):
    return jnp.broadcast_to(x[:, c : c + 1], x.shape)


def times(x, n):
    return x if n == 1 else jnp.concatenate([x] * n, axis=0)


def invert_factor(block):
    sub = lax.broadcasted_iota(jnp.int32, (TILE, BLOCK), 0)
    rows = lax.broadcasted_iota(jnp.int32, (BLOCK, BLOCK), 0)
    lanes = lax.broadcasted_iota(jnp.int32, (BLOCK, BLOCK), 1)
    ident = jnp.where(rows == lanes, 1.0, 0.0).astype(jnp.float32)
    head, rest = block[:TILE], block[TILE:]
    bhead, brest = ident[:TILE], ident[TILE:]
    done = []
    ahead = [lane_of(head, j) for j in range(TILE)]
    for s in range(TILES):
        left = TILES - 1 - s
        first = TILE * s
        col = ahead
        if left:
            below = [lane_of(rest, first + j) for j in range(TILE)]
            ahead = [lane_of(rest[:TILE], first + TILE + j) for j in range(TILE)]
        r, b = head, bhead
        scale, coef = [], {}
        for j in range(TILE):
            scale.append(lax.rsqrt(row_of(col[j], j)))
            line = col[j] * scale[j]
            for k in range(j + 1, TILE):
                coef[j, k] = row_of(line, k)
                col[k] = col[k] - line * coef[j, k]
            ru, bu = row_of(r, j) * scale[j], row_of(b, j) * scale[j]
            if j < TILE - 1:
                low = jnp.where(sub > j, line, 0.0)
                r = jnp.where(sub == j, ru, r - low * ru)
                b = jnp.where(sub == j, bu, b - low * bu)
            else:
                r = jnp.where(sub == j, ru, r)
                b = jnp.where(sub == j, bu, b)
        done.append(b)
        if not left:
            break
        lines = []
        for j in range(TILE):
            line = below[j] * times(scale[j], left)
            lines.append(line)
            for k in range(j + 1, TILE):
                below[k] = below[k] - line * times(coef[j, k], left)
        for m in range(TILE):
            near = lines[m][:TILE]
            for j in range(TILE):
                ahead[j] = ahead[j] - near * row_of(near, j)
        for j in range(TILE):
            rest = rest - lines[j] * times(row_of(r, j), left)
            brest = brest - lines[j] * times(row_of(b, j), left)
        head, rest = rest[:TILE], rest[TILE:]
        bhead, brest = brest[:TILE], brest[TILE:]
    return jnp.concatenate(done, axis=0)


def split(x):
    high = x.astype(jnp.bfloat16)
    return high, (x - high.astype(jnp.float32)).astype(jnp.bfloat16)


NN = (((1,), (0,)), ((), ()))
TN = (((0,), (0,)), ((), ()))
NT = (((1,), (1,)), ((), ()))


def dot3(a, b, dims):
    one = functools.partial(lax.dot_general, dimension_numbers=dims, preferred_element_type=jnp.float32)
    return one(a[0], b[0]) + one(a[0], b[1]) + one(a[1], b[0])


def kernel(t_ref, out, ap, aq, wb, tv, lpf, xh, xl, gx, lph, lpl, lqh, lql, diag, lsem, osem, *sems):
    net = Links(ap, aq, wb, *sems)
    p, q = net.p, net.q
    barrier = pltpu.get_barrier_semaphore()
    for device in net.neighbours():
        pl.semaphore_signal(barrier, inc=1, device_id=device, device_id_type=pl.DeviceIdType.MESH)
    cols = pl.ds(0, BLOCK)
    head = pltpu.make_async_copy(t_ref.at[cols, cols], ap.at[q % STEPS, cols], lsem.at[0])
    later = pl.ds(BLOCK, WIDTH - BLOCK)
    body = pltpu.make_async_copy(t_ref.at[later, cols], ap.at[q % STEPS, later], lsem.at[1])
    rows = [
        pltpu.make_async_copy(t_ref.at[cols, pl.ds(t * BLOCK, BLOCK)], aq.at[p % STEPS, t], lsem.at[2 + t])
        for t in range(CHUNKS)
    ]
    whole = pltpu.make_async_copy(t_ref, tv, lsem.at[2 + CHUNKS])

    @pl.when(q < STEPS)
    def _():
        head.start()
        body.start()

    @pl.when(p < STEPS)
    def _():
        for row in rows:
            row.start()

    whole.start()
    pl.semaphore_wait(barrier, 14)

    @pl.when(q < STEPS)
    def _():
        head.wait()
        body.wait()

    @pl.when(p < STEPS)
    def _():
        for row in rows:
            row.wait()

    xh[...] = jnp.zeros_like(xh)
    xl[...] = jnp.zeros_like(xl)

    net.fsource()

    def first(slot, carry):
        for m in range(4):
            pl.when(net.zfirst[m] == slot)(functools.partial(net.zitem, m, 0, True))
        net.wslot(slot)
        net.zslot(slot - START + 1)
        net.qslot(slot - START)
        for stage, at in enumerate(PASS):
            pl.when(slot == at)(functools.partial(net.fpass, stage))
        return carry

    lax.fori_loop(0, BEFORE, first, 0)
    for m in range(4):
        net.ztwin(m, 0, first=True)
    for k in range(STEPS):
        @pl.when(p == k)
        def _():
            for j in range(max(k, 2), STEPS):
                wb[k, j] = ap[j, 0:BLOCK]

    for k in range(2):
        @pl.when((p == k) & (net.z == 0) & (k <= net.c))
        def _():
            wb[k, net.c] = ap[net.c, 0:BLOCK]

    def step(k, carry):
        def catch_up(slot, carry):
            net.wslot(slot)
            net.zslot(slot - START + 1)
            net.qslot(slot - START)
            return carry

        lax.fori_loop(BEFORE + k + jnp.minimum(k, EXTRA), BEFORE + k + 1 + jnp.minimum(k + 1, EXTRA), catch_up, 0)
        net.wtwin(k)
        for kk in range(STEPS):
            lo, hi = kk * BLOCK, (kk + 1) * BLOCK

            @pl.when(k == kk)
            def _():
                if kk:
                    x = (xh[:lo, :lo], xl[:lo, :lo])
                    col = split(dot3(x, split(wb[0:kk, kk].reshape(lo, BLOCK)), NN))
                    diag[...] = wb[kk, kk] - dot3(col, col, TN)
                    gx[:, :lo] = dot3(col, x, TN)
                else:
                    diag[...] = wb[0, 0]

        ih, il = split(invert_factor(diag[...]))
        for kk in range(STEPS):
            lo, hi = kk * BLOCK, (kk + 1) * BLOCK

            @pl.when(k == kk)
            def _():
                xh[lo:hi, lo:hi] = ih
                xl[lo:hi, lo:hi] = il
                if kk:
                    xh[lo:hi, :lo], xl[lo:hi, :lo] = split(-dot3((ih, il), split(gx[:, :lo]), NN))

        return carry

    lax.fori_loop(0, STEPS, step, 0)
    whole.wait()

    def spread(u, carry):
        for n in range(AFTER):
            slot = BEFORE + STEPS + EXTRA + AFTER * u + n - START
            net.zslot(slot + 1)
            net.qslot(slot)
        for m in range(4):
            pl.when(u > 0)(lambda: net.ztwin(m, 2 * u))
            net.ztwin(m, 2 * u + 1)
        mine = pl.ds(pl.multiple_of(u * WIDE, WIDE), WIDE)
        apu = split(jnp.concatenate([ap[j, mine] for j in range(STEPS)], axis=1))
        aqu = split(jnp.concatenate(
            [jnp.concatenate([aq[i, 2 * u], aq[i, 2 * u + 1]], axis=1) for i in range(STEPS)], axis=0))
        for b in range(ROUNDS):
            lo, hi = b * WIDE, (b + 1) * WIDE
            xb = (xh[lo:hi, :hi], xl[lo:hi, :hi])
            lp = dot3((apu[0][:, :hi], apu[1][:, :hi]), xb, NT)
            lpf[2 * b, mine] = lp[:, :BLOCK]
            lpf[2 * b + 1, mine] = lp[:, BLOCK:]
            lph[u, :, lo:hi], lpl[u, :, lo:hi] = split(lp)
            lqh[u, lo:hi, :], lql[u, lo:hi, :] = split(dot3(xb, (aqu[0][:hi], aqu[1][:hi]), NN))

        def cell(a, b):
            where = (pl.ds(pl.multiple_of(a * WIDE, WIDE), WIDE), pl.ds(pl.multiple_of(b * WIDE, WIDE), WIDE))
            tv[where] = tv[where] - dot3((lph[a], lpl[a]), (lqh[b], lql[b]), NN)

        def cells(v, carry):
            cell(u, v)
            cell(v, u)
            return carry

        lax.fori_loop(0, u, cells, 0)
        cell(u, u)
        return carry

    lax.fori_loop(0, ROUNDS, spread, 0)

    @pl.when(p < STEPS)
    def _():
        tv[0:BLOCK, :] = jnp.zeros((BLOCK, WIDTH), jnp.float32)

    @pl.when(q < STEPS)
    def _():
        tv[BLOCK:, 0:BLOCK] = lpf[q % STEPS, BLOCK:]
        top = lpf[q % STEPS, 0:BLOCK]
        down = lax.broadcasted_iota(jnp.int32, (BLOCK, BLOCK), 0) + p * BLOCK
        across = lax.broadcasted_iota(jnp.int32, (BLOCK, BLOCK), 1) + q * BLOCK
        tv[0:BLOCK, 0:BLOCK] = jnp.where((p >= STEPS) | (down >= across), top, 0.0)

    result = pltpu.make_async_copy(tv, out, osem)
    result.start()
    net.drain()
    result.wait()


def per_device(blocked):
    f32, bf16 = jnp.float32, jnp.bfloat16
    hbm = pl.BlockSpec(memory_space=pl.ANY)
    dma, square = pltpu.SemaphoreType.DMA, (WIDTH, WIDTH)
    return pl.pallas_call(
        kernel,
        name="factor",
        out_shape=jax.ShapeDtypeStruct(square, f32),
        in_specs=[hbm],
        out_specs=hbm,
        scratch_shapes=[
            pltpu.VMEM((STEPS, WIDTH, BLOCK), f32),
            pltpu.VMEM((STEPS, CHUNKS, BLOCK, BLOCK), f32),
            pltpu.VMEM((STEPS, STEPS, BLOCK, BLOCK), f32),
            pltpu.VMEM(square, f32),
            pltpu.VMEM((STEPS, WIDTH, BLOCK), f32),
            *(pltpu.VMEM(square, bf16) for _ in range(2)),
            pltpu.VMEM((BLOCK, WIDTH), f32),
            *(pltpu.VMEM((ROUNDS, WIDE, WIDTH), bf16) for _ in range(2)),
            *(pltpu.VMEM((ROUNDS, WIDTH, WIDE), bf16) for _ in range(2)),
            pltpu.VMEM((BLOCK, BLOCK), f32),
            dma((3 + CHUNKS,)), dma,
            dma((STEPS, CHUNKS)), dma((2, 3, 4)),
            dma((STEPS, CHUNKS)), dma((2, 4, STEPS)),
            dma((STEPS, STEPS)), dma((5, 18)), dma((14, 2)),
        ],
        compiler_params=pltpu.CompilerParams(collective_id=0, has_side_effects=True, vmem_limit_bytes=58 << 20),
    )(blocked)


def solution(mesh):
    return jax.shard_map(
        per_device,
        mesh=mesh,
        in_specs=(P("prow", "pcol"),),
        out_specs=P("prow", "pcol"),
        check_vma=False,
    )
```

```python
import functools

import jax
import jax.numpy as jnp
from jax import lax
from jax.experimental import pallas as pl
from jax.experimental.pallas import tpu as pltpu
from jax.sharding import PartitionSpec as P

BLOCK = 128
STEPS = 8
WIDTH = BLOCK * STEPS
TILE = 8
TILES = BLOCK // TILE
SIDE = 4
RING = 8
CHUNKS = 8
STAGGER = 1
BEFORE = 5
EXTRA = 2
START = 2
AFTER = 1
PASS = (1, 2, 4)
LAST_W = 11
SKEW = 2
WIDE = 2 * BLOCK
ROUNDS = WIDTH // WIDE

UP_FIRST = ((0, 1, 2, 3, 4), (1, 2, 3, 4), (2, 3, 4, 5, 6), (3, 4, 5, 6, 7))
DOWN_FIRST = ((0, 7, 6, 5), (1, 0, 7, 6, 5), (2, 1, 0, 7), (3, 2, 1, 0))
UP = ((0, 1, 2), (1, 2, 3), (2, 3, 4, 5, 6, 7), (3, 4, 5, 6, 7, 0))
DOWN = ((0, 7, 6, 5, 4, 3), (1, 0, 7, 6, 5, 4), (2, 1, 0), (3, 2, 1))


def any_of(value, choices):
    hit = value == choices[0]
    for choice in choices[1:]:
        hit = hit | (value == choice)
    return hit


def table(value, entries):
    out = jnp.int32(entries[0])
    for n, entry in enumerate(entries[1:], 1):
        out = jnp.where(value == n, jnp.int32(entry), out)
    return out


def hops(ups, downs, m):
    return [ups[m].index(z) if z in ups[m] else downs[m].index(z) for z in range(RING)]


class Links:
    def __init__(self, ap, aq, wb, zsem, zsend, qsem, qsend, wsem, wsend, fsend):
        self.ap, self.aq, self.wb = ap, aq, wb
        self.zsem, self.zsend = zsem, zsend
        self.qsem, self.qsend = qsem, qsend
        self.wsem, self.wsend, self.fsend = wsem, wsend, fsend
        self.p, self.q = lax.axis_index("prow"), lax.axis_index("pcol")
        self.y, self.x = self.p // SIDE, self.p % SIDE
        self.z, self.c = self.q // 2, self.q % 2
        self.zhops = [table(self.z, hops(UP, DOWN, m)) for m in range(4)]
        self.zfirst = [table(self.z, hops(UP_FIRST, DOWN_FIRST, m)) for m in range(4)]
        self.up = [any_of(self.z, UP[m][:-1]) for m in range(4)]
        self.down = [any_of(self.z, DOWN[m][:-1]) for m in range(4)]
        self.up_first = [any_of(self.z, UP_FIRST[m][:-1]) for m in range(4)]
        self.down_first = [any_of(self.z, DOWN_FIRST[m][:-1]) for m in range(4)]
        self.beside = (self.device(dy=1), self.device(dy=3), self.device(dx=1), self.device(dx=3))
        self.along = (self.device(dz=1), self.device(dz=RING - 1), self.device(dc=1))
        self.qhops, self.ways = [], []
        for i in range(STEPS):
            ys, dx = i // SIDE, (self.x - i % SIDE + SIDE) % SIDE
            row, same = self.y == ys, dx == 0
            self.qhops.append(table(self.y, (0, 1, 2, 1) if ys == 0 else (1, 0, 1, 2)) + table(dx, (0, 1, 2, 1)))
            turn = row | (self.y == (3 if ys == 0 else 2))
            on = same | (dx == (1 if ys == 0 else 3))
            ways = []
            for down, across in ((same, True), (True, row)):
                one, two = (row & down, turn & down), (on & across, same & across)
                ways.append((*(one if ys == 0 else one[::-1]), *(two if ys == 0 else two[::-1])))
            self.ways.append(ways)

    def device(self, dx=0, dy=0, dz=0, dc=0):
        prow = (self.y + dy) % SIDE * SIDE + (self.x + dx) % SIDE
        pcol = (self.z + dz) % RING * 2 + (self.c + dc) % 2
        return (prow, pcol)

    def neighbours(self):
        around = [self.device(dx=n) for n in (1, 2, 3)] + [self.device(dy=n) for n in (1, 2, 3)]
        return around + [self.device(dz=n) for n in range(1, RING)] + [self.device(dc=1)]

    def copy(self, src, dst, send, recv, device):
        return pltpu.make_async_remote_copy(
            src_ref=src, dst_ref=dst, send_sem=send, recv_sem=recv,
            device_id=device, device_id_type=pl.DeviceIdType.MESH,
        )

    def zcopy(self, way, m, t, parity, first=False):
        j = 2 * m + parity
        part = self.ap.at[j, pl.ds(0 if first else pl.multiple_of(t * BLOCK, BLOCK), BLOCK)]
        return self.copy(part, part, self.zsend.at[int(first), way, m], self.zsem.at[j, t], self.along[way])

    def zitem(self, m, t, first=False):
        up, down = (self.up_first, self.down_first) if first else (self.up, self.down)

        @pl.when(self.z != m)
        def _():
            self.zcopy(0, m, t, self.c, first).wait_recv()

        for way, sends in enumerate((up[m], down[m])):
            @pl.when(sends)
            def _():
                self.zcopy(way, m, t, self.c, first).start()

        self.zcopy(2, m, t, self.c, first).start()

    def zslot(self, slot):
        for m in range(4):
            t = slot - SKEW * self.zhops[m]

            @pl.when((t >= 1) & (t < CHUNKS))
            def _():
                self.zitem(m, t)

    def ztwin(self, m, t, first=False):
        self.zcopy(2, m, t, 1 - self.c, first).wait_recv()

    def qcopy(self, way, i, t, order=0):
        part = self.aq.at[i, t]
        return self.copy(part, part, self.qsend.at[order, way, i], self.qsem.at[i, t], self.beside[way])

    def qslot(self, slot):
        for i in range(STEPS):
            t = slot - SKEW * self.qhops[i]

            @pl.when((t >= 0) & (t < CHUNKS))
            def _():
                @pl.when(self.p != i)
                def _():
                    self.qcopy(0, i, t).wait_recv()

                odd = t % 2
                for way, (even_sends, odd_sends) in enumerate(zip(*self.ways[i])):
                    @pl.when(jnp.where(odd == 1, odd_sends, even_sends))
                    def _():
                        self.qcopy(way, i, t, odd).start()

    def wcopy(self, way, k, m, parity, own=False):
        device = self.along[2] if way == 4 else self.beside[way]
        j = 2 * m + parity
        dst = self.wb.at[k, j]
        src = self.ap.at[j, pl.ds(0, BLOCK)] if own else dst
        send = self.wsend.at[way, m * (m + 1) - 2 + k]
        return self.copy(src, dst, send, self.wsem.at[k, j], device)

    def wneeded(self, k, m):
        return self.c == 1 if k == 2 * m + 1 else self.c >= 0

    def wslot(self, slot):
        for m in range(1, 4):
            for k in range(2 * m + 2):
                @pl.when((self.zfirst[m] + self.qhops[k] + STAGGER * (m - 1) == slot) & self.wneeded(k, m))
                def _():
                    @pl.when(self.p == k)
                    def _():
                        for way in range(4):
                            pl.when(self.ways[k][0][way])(self.wcopy(way, k, m, self.c, own=True).start)

                    @pl.when(self.p != k)
                    def _():
                        self.wcopy(0, k, m, self.c).wait_recv()
                        for way in range(4):
                            pl.when(self.ways[k][0][way])(self.wcopy(way, k, m, self.c).start)
                        self.wcopy(4, k, m, self.c).start()

    def fcopy(self, n, k, parity, own=False):
        if n < 7:
            device = self.device(dz=(4, 3, 5, 2, 6, 1, 7)[n])
        elif n < 13:
            step = (2, 1, 3)[(n - 7) % 3]
            device = self.device(dy=step) if n < 10 else self.device(dx=step)
        else:
            device = self.along[2]
        dst = self.wb.at[k, parity]
        src = self.ap.at[parity, pl.ds(0, BLOCK)] if own else dst
        return self.copy(src, dst, self.fsend.at[n, k], self.wsem.at[k, parity], device)

    def fsource(self):
        for k in range(2):
            @pl.when((self.p == k) & (self.z == 0) & (k <= self.c))
            def _():
                for n in range(14):
                    self.fcopy(n, k, self.c, own=True).start()

    def fpass(self, stage):
        for k in range(2):
            needed = k <= self.c
            if stage == 0:
                here, sends = (self.p == k) & (self.z != 0), range(7, 14)
            elif stage == 1:
                here, sends = (self.x == k) & (self.y != 0), range(10, 14)
            else:
                here, sends = self.x != k, range(13, 14)

            @pl.when(here & needed)
            def _():
                self.fcopy(0, k, self.c).wait_recv()
                for n in sends:
                    self.fcopy(n, k, self.c).start()

    def wtwin(self, j):
        @pl.when(self.c != j % 2)
        def _():
            def item(k, carry):
                part = self.wb.at[k, j]
                twin = self.copy(part, part, self.fsend.at[0, 0], self.wsem.at[k, j], self.along[2])
                pl.when((j < 2) | (self.p != k))(twin.wait_recv)
                return carry

            lax.fori_loop(0, j + 1, item, 0)

    def drain(self):
        for m in range(4):
            for way, first, later in (
                (0, self.up_first[m], self.up[m]), (1, self.down_first[m], self.down[m]), (2, None, None),
            ):
                device = self.device(dc=1)
                one, rest = self.ap.at[0, pl.ds(0, BLOCK)], self.ap.at[0, pl.ds(0, WIDTH - BLOCK)]
                head = self.copy(one, one, self.zsend.at[1, way, m], self.zsem.at[0, 0], device)
                tail = self.copy(rest, rest, self.zsend.at[0, way, m], self.zsem.at[0, 0], device)
                if first is None:
                    head.wait_send()
                    tail.wait_send()
                else:
                    pl.when(first)(head.wait_send)
                    pl.when(later)(tail.wait_send)
        for i in range(STEPS):
            half = self.aq.at[i, pl.ds(0, CHUNKS // 2)]
            for order in range(2):
                for way, sends in enumerate(self.ways[i][order]):
                    every = self.copy(half, half, self.qsend.at[order, way, i], self.qsem.at[0, 0], self.beside[way])
                    pl.when(sends)(every.wait_send)
        for m in range(1, 4):
            for k in range(2 * m + 2):
                for way in range(5):
                    sends = self.ways[k][0][way] if way < 4 else self.p != k
                    pl.when(sends & self.wneeded(k, m))(self.wcopy(way, k, m, self.c).wait_send)
        for k in range(2):
            for n in range(14):
                line = (self.p == k) & (self.z == 0) if n < 7 else self.p == k if n < 10 else self.x == k if n < 13 else True
                pl.when(line & (k <= self.c))(self.fcopy(n, k, self.c).wait_send)


def row_of(x, j):
    return jnp.broadcast_to(x[j : j + 1, :], (TILE, BLOCK))


def lane_of(x, c):
    return jnp.broadcast_to(x[:, c : c + 1], x.shape)


def times(x, n):
    return x if n == 1 else jnp.concatenate([x] * n, axis=0)


def invert_factor(block):
    sub = lax.broadcasted_iota(jnp.int32, (TILE, BLOCK), 0)
    rows = lax.broadcasted_iota(jnp.int32, (BLOCK, BLOCK), 0)
    lanes = lax.broadcasted_iota(jnp.int32, (BLOCK, BLOCK), 1)
    ident = jnp.where(rows == lanes, 1.0, 0.0).astype(jnp.float32)
    head, rest = block[:TILE], block[TILE:]
    bhead, brest = ident[:TILE], ident[TILE:]
    done = []
    ahead = [lane_of(head, j) for j in range(TILE)]
    for s in range(TILES):
        left = TILES - 1 - s
        first = TILE * s
        col = ahead
        if left:
            below = [lane_of(rest, first + j) for j in range(TILE)]
            ahead = [lane_of(rest[:TILE], first + TILE + j) for j in range(TILE)]
        r, b = head, bhead
        scale, coef = [], {}
        for j in range(TILE):
            scale.append(lax.rsqrt(row_of(col[j], j)))
            line = col[j] * scale[j]
            for k in range(j + 1, TILE):
                coef[j, k] = row_of(line, k)
                col[k] = col[k] - line * coef[j, k]
            ru, bu = row_of(r, j) * scale[j], row_of(b, j) * scale[j]
            if j < TILE - 1:
                low = jnp.where(sub > j, line, 0.0)
                r = jnp.where(sub == j, ru, r - low * ru)
                b = jnp.where(sub == j, bu, b - low * bu)
            else:
                r = jnp.where(sub == j, ru, r)
                b = jnp.where(sub == j, bu, b)
        done.append(b)
        if not left:
            break
        lines = []
        for j in range(TILE):
            line = below[j] * times(scale[j], left)
            lines.append(line)
            for k in range(j + 1, TILE):
                below[k] = below[k] - line * times(coef[j, k], left)
        for m in range(TILE):
            near = lines[m][:TILE]
            for j in range(TILE):
                ahead[j] = ahead[j] - near * row_of(near, j)
        for j in range(TILE):
            rest = rest - lines[j] * times(row_of(r, j), left)
            brest = brest - lines[j] * times(row_of(b, j), left)
        head, rest = rest[:TILE], rest[TILE:]
        bhead, brest = brest[:TILE], brest[TILE:]
    return jnp.concatenate(done, axis=0)


def split(x):
    high = x.astype(jnp.bfloat16)
    return high, (x - high.astype(jnp.float32)).astype(jnp.bfloat16)


NN = (((1,), (0,)), ((), ()))
TN = (((0,), (0,)), ((), ()))
NT = (((1,), (1,)), ((), ()))


def dot3(a, b, dims):
    one = functools.partial(lax.dot_general, dimension_numbers=dims, preferred_element_type=jnp.float32)
    return one(a[0], b[0]) + one(a[0], b[1]) + one(a[1], b[0])


def kernel(t_ref, out, ap, aq, wb, tv, lpf, xh, xl, gx, colh, coll, lph, lpl, lqh, lql, diag, lsem, osem, *sems):
    net = Links(ap, aq, wb, *sems)
    p, q = net.p, net.q
    barrier = pltpu.get_barrier_semaphore()
    for device in net.neighbours():
        pl.semaphore_signal(barrier, inc=1, device_id=device, device_id_type=pl.DeviceIdType.MESH)
    cols = pl.ds(0, BLOCK)
    head = pltpu.make_async_copy(t_ref.at[cols, cols], ap.at[q % STEPS, cols], lsem.at[0])
    later = pl.ds(BLOCK, WIDTH - BLOCK)
    body = pltpu.make_async_copy(t_ref.at[later, cols], ap.at[q % STEPS, later], lsem.at[1])
    rows = [
        pltpu.make_async_copy(t_ref.at[cols, pl.ds(t * BLOCK, BLOCK)], aq.at[p % STEPS, t], lsem.at[2 + t])
        for t in range(CHUNKS)
    ]
    whole = pltpu.make_async_copy(t_ref, tv, lsem.at[2 + CHUNKS])

    @pl.when(q < STEPS)
    def _():
        head.start()
        body.start()

    @pl.when(p < STEPS)
    def _():
        for row in rows:
            row.start()

    whole.start()
    xh[...] = jnp.zeros_like(xh)
    xl[...] = jnp.zeros_like(xl)
    gx[...] = jnp.zeros_like(gx)
    colh[...] = jnp.zeros_like(colh)
    coll[...] = jnp.zeros_like(coll)

    for k in range(1, STEPS):
        for j in range(k):
            wb[k, j] = jnp.zeros((BLOCK, BLOCK), jnp.float32)

    pl.semaphore_wait(barrier, 14)

    @pl.when(q < STEPS)
    def _():
        head.wait()
        body.wait()

    @pl.when(p < STEPS)
    def _():
        for row in rows:
            row.wait()

    net.fsource()

    def first(slot, carry):
        for m in range(4):
            pl.when(net.zfirst[m] == slot)(functools.partial(net.zitem, m, 0, True))
        net.wslot(slot)
        net.zslot(slot - START + 1)
        net.qslot(slot - START)
        for stage, at in enumerate(PASS):
            pl.when(slot == at)(functools.partial(net.fpass, stage))
        return carry

    lax.fori_loop(0, BEFORE, first, 0)
    for m in range(4):
        net.ztwin(m, 0, first=True)
    for k in range(STEPS):
        @pl.when(p == k)
        def _():
            for j in range(max(k, 2), STEPS):
                wb[k, j] = ap[j, 0:BLOCK]

    for k in range(2):
        @pl.when((p == k) & (net.z == 0) & (k <= net.c))
        def _():
            wb[k, net.c] = ap[net.c, 0:BLOCK]

    def step(known, k, carry):
        def catch_up(slot, carry):
            pl.when(slot < LAST_W)(lambda: net.wslot(slot))

            @pl.when((slot >= START) & (slot < START + CHUNKS + 5 * SKEW))
            def _():
                net.zslot(slot - START + 1)
                net.qslot(slot - START)

            return carry

        lax.fori_loop(BEFORE + k + jnp.minimum(k, EXTRA), BEFORE + k + 1 + jnp.minimum(k + 1, EXTRA), catch_up, 0)

        @pl.when(k == 0)
        def _():
            net.wtwin(0)
            diag[...] = wb[0, 0]

        if known:
            net.wtwin(k + 1)
            full = slice(0, known)
            x = (xh[full, full], xl[full, full])
            part = split(dot3(x, split(wb[0 : known // BLOCK, k + 1].reshape(known, BLOCK)), NN))
            cross = dot3((colh[full], coll[full]), part, TN)
            square = dot3(part, part, TN)
            across = dot3(part, x, TN)
        inv = split(invert_factor(diag[...]))
        mine = pl.ds(pl.multiple_of(k * BLOCK, BLOCK), BLOCK)
        row = split(-dot3(inv, split(gx[...]), NN))
        xh[mine, :], xl[mine, :] = row
        xh[mine, mine], xl[mine, mine] = inv
        if known:
            last = split(dot3(inv, split(wb[k, k + 1] - cross), NN))
            diag[...] = wb[k + 1, k + 1] - square - dot3(last, last, TN)
            colh[full], coll[full] = part
            colh[mine], coll[mine] = last
            gx[...] = dot3(last, (xh[mine, :], xl[mine, :]), TN)
            gx[:, full] = gx[:, full] + across
        return carry

    lax.fori_loop(0, 5, functools.partial(step, 4 * BLOCK), 0)
    lax.fori_loop(5, 7, functools.partial(step, 6 * BLOCK), 0)
    step(0, jnp.int32(7), 0)
    whole.wait()

    def spread(u, carry):
        for n in range(AFTER):
            slot = BEFORE + STEPS + EXTRA + AFTER * u + n - START
            net.zslot(slot + 1)
            net.qslot(slot)
        for m in range(4):
            pl.when(u > 0)(lambda: net.ztwin(m, 2 * u))
            net.ztwin(m, 2 * u + 1)
        mine = pl.ds(pl.multiple_of(u * WIDE, WIDE), WIDE)
        apu = split(jnp.concatenate([ap[j, mine] for j in range(STEPS)], axis=1))
        aqu = split(jnp.concatenate(
            [jnp.concatenate([aq[i, 2 * u], aq[i, 2 * u + 1]], axis=1) for i in range(STEPS)], axis=0))
        for b in range(ROUNDS):
            lo, hi = b * WIDE, (b + 1) * WIDE
            xb = (xh[lo:hi, :hi], xl[lo:hi, :hi])
            lp = dot3((apu[0][:, :hi], apu[1][:, :hi]), xb, NT)
            lpf[2 * b, mine] = lp[:, :BLOCK]
            lpf[2 * b + 1, mine] = lp[:, BLOCK:]
            lph[u, :, lo:hi], lpl[u, :, lo:hi] = split(lp)
            lqh[u, lo:hi, :], lql[u, lo:hi, :] = split(dot3(xb, (aqu[0][:hi], aqu[1][:hi]), NN))

        def cell(a, b):
            where = (pl.ds(pl.multiple_of(a * WIDE, WIDE), WIDE), pl.ds(pl.multiple_of(b * WIDE, WIDE), WIDE))
            tv[where] = tv[where] - dot3((lph[a], lpl[a]), (lqh[b], lql[b]), NN)

        def cells(v, carry):
            cell(u, v)
            cell(v, u)
            return carry

        lax.fori_loop(0, u, cells, 0)
        cell(u, u)
        return carry

    lax.fori_loop(0, ROUNDS, spread, 0)

    @pl.when(p < STEPS)
    def _():
        tv[0:BLOCK, :] = jnp.zeros((BLOCK, WIDTH), jnp.float32)

    @pl.when(q < STEPS)
    def _():
        tv[BLOCK:, 0:BLOCK] = lpf[q % STEPS, BLOCK:]
        top = lpf[q % STEPS, 0:BLOCK]
        down = lax.broadcasted_iota(jnp.int32, (BLOCK, BLOCK), 0) + p * BLOCK
        across = lax.broadcasted_iota(jnp.int32, (BLOCK, BLOCK), 1) + q * BLOCK
        tv[0:BLOCK, 0:BLOCK] = jnp.where((p >= STEPS) | (down >= across), top, 0.0)

    result = pltpu.make_async_copy(tv, out, osem)
    result.start()
    net.drain()
    result.wait()


def per_device(blocked):
    f32, bf16 = jnp.float32, jnp.bfloat16
    hbm = pl.BlockSpec(memory_space=pl.ANY)
    dma, square = pltpu.SemaphoreType.DMA, (WIDTH, WIDTH)
    return pl.pallas_call(
        kernel,
        name="factor",
        out_shape=jax.ShapeDtypeStruct(square, f32),
        in_specs=[hbm],
        out_specs=hbm,
        scratch_shapes=[
            pltpu.VMEM((STEPS, WIDTH, BLOCK), f32),
            pltpu.VMEM((STEPS, CHUNKS, BLOCK, BLOCK), f32),
            pltpu.VMEM((STEPS, STEPS, BLOCK, BLOCK), f32),
            pltpu.VMEM(square, f32),
            pltpu.VMEM((STEPS, WIDTH, BLOCK), f32),
            *(pltpu.VMEM(square, bf16) for _ in range(2)),
            pltpu.VMEM((BLOCK, WIDTH), f32),
            *(pltpu.VMEM((WIDTH, BLOCK), bf16) for _ in range(2)),
            *(pltpu.VMEM((ROUNDS, WIDE, WIDTH), bf16) for _ in range(2)),
            *(pltpu.VMEM((ROUNDS, WIDTH, WIDE), bf16) for _ in range(2)),
            pltpu.VMEM((BLOCK, BLOCK), f32),
            dma((3 + CHUNKS,)), dma,
            dma((STEPS, CHUNKS)), dma((2, 3, 4)),
            dma((STEPS, CHUNKS)), dma((2, 4, STEPS)),
            dma((STEPS, STEPS)), dma((5, 18)), dma((14, 2)),
        ],
        compiler_params=pltpu.CompilerParams(collective_id=0, has_side_effects=True, vmem_limit_bytes=58 << 20),
    )(blocked)


def solution(mesh):
    return jax.shard_map(
        per_device,
        mesh=mesh,
        in_specs=(P("prow", "pcol"),),
        out_specs=P("prow", "pcol"),
        check_vma=False,
    )
```

```python
import functools

import jax
import jax.numpy as jnp
from jax import lax
from jax.experimental import pallas as pl
from jax.experimental.pallas import tpu as pltpu
from jax.sharding import PartitionSpec as P

BLOCK = 128
STEPS = 8
WIDTH = BLOCK * STEPS
TILE = 8
TILES = BLOCK // TILE
SIDE = 4
RING = 8
CHUNKS = 8
STAGGER = 1
BEFORE = 5
EXTRA = 2
START = 2
AFTER = 1
PASS = (1, 2, 4)
LAST_W = 11
SKEW = 2
WIDE = 2 * BLOCK
ROUNDS = WIDTH // WIDE

UP_FIRST = ((0, 1, 2, 3, 4), (1, 2, 3, 4), (2, 3, 4, 5, 6), (3, 4, 5, 6, 7))
DOWN_FIRST = ((0, 7, 6, 5), (1, 0, 7, 6, 5), (2, 1, 0, 7), (3, 2, 1, 0))
UP = ((0, 1, 2), (1, 2, 3), (2, 3, 4, 5, 6, 7), (3, 4, 5, 6, 7, 0))
DOWN = ((0, 7, 6, 5, 4, 3), (1, 0, 7, 6, 5, 4), (2, 1, 0), (3, 2, 1))


def any_of(value, choices):
    hit = value == choices[0]
    for choice in choices[1:]:
        hit = hit | (value == choice)
    return hit


def table(value, entries):
    out = jnp.int32(entries[0])
    for n, entry in enumerate(entries[1:], 1):
        out = jnp.where(value == n, jnp.int32(entry), out)
    return out


def hops(ups, downs, m):
    return [ups[m].index(z) if z in ups[m] else downs[m].index(z) for z in range(RING)]


class Links:
    def __init__(self, ap, aq, wb, zsem, zsend, qsem, qsend, wsem, wsend, fsend):
        self.ap, self.aq, self.wb = ap, aq, wb
        self.zsem, self.zsend = zsem, zsend
        self.qsem, self.qsend = qsem, qsend
        self.wsem, self.wsend, self.fsend = wsem, wsend, fsend
        self.p, self.q = lax.axis_index("prow"), lax.axis_index("pcol")
        self.y, self.x = self.p // SIDE, self.p % SIDE
        self.z, self.c = self.q // 2, self.q % 2
        self.zhops = [table(self.z, hops(UP, DOWN, m)) for m in range(4)]
        self.zfirst = [table(self.z, hops(UP_FIRST, DOWN_FIRST, m)) for m in range(4)]
        self.up = [any_of(self.z, UP[m][:-1]) for m in range(4)]
        self.down = [any_of(self.z, DOWN[m][:-1]) for m in range(4)]
        self.up_first = [any_of(self.z, UP_FIRST[m][:-1]) for m in range(4)]
        self.down_first = [any_of(self.z, DOWN_FIRST[m][:-1]) for m in range(4)]
        self.beside = (self.device(dy=1), self.device(dy=3), self.device(dx=1), self.device(dx=3))
        self.along = (self.device(dz=1), self.device(dz=RING - 1), self.device(dc=1))
        self.qhops, self.ways = [], []
        for i in range(STEPS):
            ys, dx = i // SIDE, (self.x - i % SIDE + SIDE) % SIDE
            row, same = self.y == ys, dx == 0
            self.qhops.append(table(self.y, (0, 1, 2, 1) if ys == 0 else (1, 0, 1, 2)) + table(dx, (0, 1, 2, 1)))
            turn = row | (self.y == (3 if ys == 0 else 2))
            on = same | (dx == (1 if ys == 0 else 3))
            ways = []
            for down, across in ((same, True), (True, row)):
                one, two = (row & down, turn & down), (on & across, same & across)
                ways.append((*(one if ys == 0 else one[::-1]), *(two if ys == 0 else two[::-1])))
            self.ways.append(ways)

    def device(self, dx=0, dy=0, dz=0, dc=0):
        prow = (self.y + dy) % SIDE * SIDE + (self.x + dx) % SIDE
        pcol = (self.z + dz) % RING * 2 + (self.c + dc) % 2
        return (prow, pcol)

    def neighbours(self):
        around = [self.device(dx=n) for n in (1, 2, 3)] + [self.device(dy=n) for n in (1, 2, 3)]
        return around + [self.device(dz=n) for n in range(1, RING)] + [self.device(dc=1)]

    def copy(self, src, dst, send, recv, device):
        return pltpu.make_async_remote_copy(
            src_ref=src, dst_ref=dst, send_sem=send, recv_sem=recv,
            device_id=device, device_id_type=pl.DeviceIdType.MESH,
        )

    def zcopy(self, way, m, t, parity, first=False):
        j = 2 * m + parity
        part = self.ap.at[j, pl.ds(0 if first else pl.multiple_of(t * BLOCK, BLOCK), BLOCK)]
        return self.copy(part, part, self.zsend.at[int(first), way, m], self.zsem.at[j, t], self.along[way])

    def zitem(self, m, t, first=False):
        up, down = (self.up_first, self.down_first) if first else (self.up, self.down)

        @pl.when(self.z != m)
        def _():
            self.zcopy(0, m, t, self.c, first).wait_recv()

        for way, sends in enumerate((up[m], down[m])):
            @pl.when(sends)
            def _():
                self.zcopy(way, m, t, self.c, first).start()

        self.zcopy(2, m, t, self.c, first).start()

    def zslot(self, slot):
        for m in range(4):
            t = slot - SKEW * self.zhops[m]

            @pl.when((t >= 1) & (t < CHUNKS))
            def _():
                self.zitem(m, t)

    def ztwin(self, m, t, first=False):
        self.zcopy(2, m, t, 1 - self.c, first).wait_recv()

    def qcopy(self, way, i, t, order=0):
        part = self.aq.at[i, t]
        return self.copy(part, part, self.qsend.at[order, way, i], self.qsem.at[i, t], self.beside[way])

    def qslot(self, slot):
        for i in range(STEPS):
            t = slot - SKEW * self.qhops[i]

            @pl.when((t >= 0) & (t < CHUNKS))
            def _():
                @pl.when(self.p != i)
                def _():
                    self.qcopy(0, i, t).wait_recv()

                odd = t % 2
                for way, (even_sends, odd_sends) in enumerate(zip(*self.ways[i])):
                    @pl.when(jnp.where(odd == 1, odd_sends, even_sends))
                    def _():
                        self.qcopy(way, i, t, odd).start()

    def wcopy(self, way, k, m, parity, own=False):
        device = self.along[2] if way == 4 else self.beside[way]
        j = 2 * m + parity
        dst = self.wb.at[k, j]
        src = self.ap.at[j, pl.ds(0, BLOCK)] if own else dst
        send = self.wsend.at[way, m * (m + 1) - 2 + k]
        return self.copy(src, dst, send, self.wsem.at[k, j], device)

    def wneeded(self, k, m):
        return self.c == 1 if k == 2 * m + 1 else self.c >= 0

    def wslot(self, slot):
        for m in range(1, 4):
            for k in range(2 * m + 2):
                @pl.when((self.zfirst[m] + self.qhops[k] + STAGGER * (m - 1) == slot) & self.wneeded(k, m))
                def _():
                    @pl.when(self.p == k)
                    def _():
                        for way in range(4):
                            pl.when(self.ways[k][0][way])(self.wcopy(way, k, m, self.c, own=True).start)

                    @pl.when(self.p != k)
                    def _():
                        self.wcopy(0, k, m, self.c).wait_recv()
                        for way in range(4):
                            pl.when(self.ways[k][0][way])(self.wcopy(way, k, m, self.c).start)
                        self.wcopy(4, k, m, self.c).start()

    def fcopy(self, n, k, parity, own=False):
        if n < 7:
            device = self.device(dz=(4, 3, 5, 2, 6, 1, 7)[n])
        elif n < 13:
            step = (2, 1, 3)[(n - 7) % 3]
            device = self.device(dy=step) if n < 10 else self.device(dx=step)
        else:
            device = self.along[2]
        dst = self.wb.at[k, parity]
        src = self.ap.at[parity, pl.ds(0, BLOCK)] if own else dst
        return self.copy(src, dst, self.fsend.at[n, k], self.wsem.at[k, parity], device)

    def fsource(self):
        for k in range(2):
            @pl.when((self.p == k) & (self.z == 0) & (k <= self.c))
            def _():
                for n in range(14):
                    self.fcopy(n, k, self.c, own=True).start()

    def fpass(self, stage):
        for k in range(2):
            needed = k <= self.c
            if stage == 0:
                here, sends = (self.p == k) & (self.z != 0), range(7, 14)
            elif stage == 1:
                here, sends = (self.x == k) & (self.y != 0), range(10, 14)
            else:
                here, sends = self.x != k, range(13, 14)

            @pl.when(here & needed)
            def _():
                self.fcopy(0, k, self.c).wait_recv()
                for n in sends:
                    self.fcopy(n, k, self.c).start()

    def wtwin(self, j):
        @pl.when(self.c != j % 2)
        def _():
            def item(k, carry):
                part = self.wb.at[k, j]
                twin = self.copy(part, part, self.fsend.at[0, 0], self.wsem.at[k, j], self.along[2])
                pl.when((j < 2) | (self.p != k))(twin.wait_recv)
                return carry

            lax.fori_loop(0, j + 1, item, 0)

    def drain(self):
        for m in range(4):
            for way, first, later in (
                (0, self.up_first[m], self.up[m]), (1, self.down_first[m], self.down[m]), (2, None, None),
            ):
                device = self.device(dc=1)
                one, rest = self.ap.at[0, pl.ds(0, BLOCK)], self.ap.at[0, pl.ds(0, WIDTH - BLOCK)]
                head = self.copy(one, one, self.zsend.at[1, way, m], self.zsem.at[0, 0], device)
                tail = self.copy(rest, rest, self.zsend.at[0, way, m], self.zsem.at[0, 0], device)
                if first is None:
                    head.wait_send()
                    tail.wait_send()
                else:
                    pl.when(first)(head.wait_send)
                    pl.when(later)(tail.wait_send)
        for i in range(STEPS):
            half = self.aq.at[i, pl.ds(0, CHUNKS // 2)]
            for order in range(2):
                for way, sends in enumerate(self.ways[i][order]):
                    every = self.copy(half, half, self.qsend.at[order, way, i], self.qsem.at[0, 0], self.beside[way])
                    pl.when(sends)(every.wait_send)
        for m in range(1, 4):
            for k in range(2 * m + 2):
                for way in range(5):
                    sends = self.ways[k][0][way] if way < 4 else self.p != k
                    pl.when(sends & self.wneeded(k, m))(self.wcopy(way, k, m, self.c).wait_send)
        for k in range(2):
            for n in range(14):
                line = (self.p == k) & (self.z == 0) if n < 7 else self.p == k if n < 10 else self.x == k if n < 13 else True
                pl.when(line & (k <= self.c))(self.fcopy(n, k, self.c).wait_send)


def row_of(x, j):
    return jnp.broadcast_to(x[j : j + 1, :], (TILE, BLOCK))


def lane_of(x, c):
    return jnp.broadcast_to(x[:, c : c + 1], x.shape)


def times(x, n):
    return x if n == 1 else jnp.concatenate([x] * n, axis=0)


def invert_factor(block):
    sub = lax.broadcasted_iota(jnp.int32, (TILE, BLOCK), 0)
    rows = lax.broadcasted_iota(jnp.int32, (BLOCK, BLOCK), 0)
    lanes = lax.broadcasted_iota(jnp.int32, (BLOCK, BLOCK), 1)
    ident = jnp.where(rows == lanes, 1.0, 0.0).astype(jnp.float32)
    head, rest = block[:TILE], block[TILE:]
    bhead, brest = ident[:TILE], ident[TILE:]
    done = []
    ahead = [lane_of(head, j) for j in range(TILE)]
    for s in range(TILES):
        left = TILES - 1 - s
        first = TILE * s
        col = ahead
        if left:
            below = [lane_of(rest, first + j) for j in range(TILE)]
            ahead = [lane_of(rest[:TILE], first + TILE + j) for j in range(TILE)]
        r, b = head, bhead
        scale, coef = [], {}
        for j in range(TILE):
            scale.append(lax.rsqrt(row_of(col[j], j)))
            line = col[j] * scale[j]
            for k in range(j + 1, TILE):
                coef[j, k] = row_of(line, k)
                col[k] = col[k] - line * coef[j, k]
            ru, bu = row_of(r, j) * scale[j], row_of(b, j) * scale[j]
            if j < TILE - 1:
                low = jnp.where(sub > j, line, 0.0)
                r = jnp.where(sub == j, ru, r - low * ru)
                b = jnp.where(sub == j, bu, b - low * bu)
            else:
                r = jnp.where(sub == j, ru, r)
                b = jnp.where(sub == j, bu, b)
        done.append(b)
        if not left:
            break
        lines = []
        for j in range(TILE):
            line = below[j] * times(scale[j], left)
            lines.append(line)
            for k in range(j + 1, TILE):
                below[k] = below[k] - line * times(coef[j, k], left)
        for m in range(TILE):
            near = lines[m][:TILE]
            for j in range(TILE):
                ahead[j] = ahead[j] - near * row_of(near, j)
        for j in range(TILE):
            rest = rest - lines[j] * times(row_of(r, j), left)
            brest = brest - lines[j] * times(row_of(b, j), left)
        head, bhead = rest[:TILE], brest[:TILE]
        if left > 1:
            rest, brest = rest[TILE:], brest[TILE:]
    return jnp.concatenate(done, axis=0)


def split(x):
    high = x.astype(jnp.bfloat16)
    return high, (x - high.astype(jnp.float32)).astype(jnp.bfloat16)


NN = (((1,), (0,)), ((), ()))
TN = (((0,), (0,)), ((), ()))
NT = (((1,), (1,)), ((), ()))


def dot3(a, b, dims):
    one = functools.partial(lax.dot_general, dimension_numbers=dims, preferred_element_type=jnp.float32)
    return one(a[0], b[0]) + one(a[0], b[1]) + one(a[1], b[0])


def kernel(t_ref, out, ap, aq, wb, tv, lpf, xh, xl, gx, colh, coll, lph, lpl, lqh, lql, diag, lsem, osem, zsem, qsem, wsem):
    dma = pltpu.SemaphoreType.DMA
    pl.run_scoped(
        functools.partial(steps, t_ref, out, ap, aq, wb, tv, lpf, xh, xl, gx, colh, coll, lph, lpl, lqh, lql, diag, lsem, osem, zsem, qsem, wsem),
        dma((2, 3, 4)), dma((2, 4, STEPS)), dma((5, 18)), dma((14, 2)),
    )


def steps(
    t_ref, out, ap, aq, wb, tv, lpf, xh, xl, gx, colh, coll, lph, lpl, lqh, lql, diag, lsem, osem, zsem, qsem, wsem,
    zsend, qsend, wsend, fsend,
):
    net = Links(ap, aq, wb, zsem, zsend, qsem, qsend, wsem, wsend, fsend)
    p, q = net.p, net.q
    barrier = pltpu.get_barrier_semaphore()
    for device in net.neighbours():
        pl.semaphore_signal(barrier, inc=1, device_id=device, device_id_type=pl.DeviceIdType.MESH)
    cols = pl.ds(0, BLOCK)
    head = pltpu.make_async_copy(t_ref.at[cols, cols], ap.at[q % STEPS, cols], lsem.at[0])
    later = pl.ds(BLOCK, WIDTH - BLOCK)
    body = pltpu.make_async_copy(t_ref.at[later, cols], ap.at[q % STEPS, later], lsem.at[1])
    rows = [
        pltpu.make_async_copy(t_ref.at[cols, pl.ds(t * BLOCK, BLOCK)], aq.at[p % STEPS, t], lsem.at[2 + t])
        for t in range(CHUNKS)
    ]
    whole = pltpu.make_async_copy(t_ref, tv, lsem.at[2 + CHUNKS])

    @pl.when(q < STEPS)
    def _():
        head.start()
        body.start()

    @pl.when(p < STEPS)
    def _():
        for row in rows:
            row.start()

    whole.start()
    xh[...] = jnp.zeros_like(xh)
    xl[...] = jnp.zeros_like(xl)
    gx[...] = jnp.zeros_like(gx)
    colh[...] = jnp.zeros_like(colh)
    coll[...] = jnp.zeros_like(coll)

    for k in range(1, STEPS):
        for j in range(k):
            wb[k, j] = jnp.zeros((BLOCK, BLOCK), jnp.float32)

    pl.semaphore_wait(barrier, 14)

    @pl.when(q < STEPS)
    def _():
        head.wait()
        body.wait()

    @pl.when(p < STEPS)
    def _():
        for row in rows:
            row.wait()

    net.fsource()

    def first(slot, carry):
        for m in range(4):
            pl.when(net.zfirst[m] == slot)(functools.partial(net.zitem, m, 0, True))
        net.wslot(slot)
        net.zslot(slot - START + 1)
        net.qslot(slot - START)
        for stage, at in enumerate(PASS):
            pl.when(slot == at)(functools.partial(net.fpass, stage))
        return carry

    lax.fori_loop(0, BEFORE, first, 0)
    for m in range(4):
        net.ztwin(m, 0, first=True)
    for k in range(STEPS):
        @pl.when(p == k)
        def _():
            for j in range(max(k, 2), STEPS):
                wb[k, j] = ap[j, 0:BLOCK]

    for k in range(2):
        @pl.when((p == k) & (net.z == 0) & (k <= net.c))
        def _():
            wb[k, net.c] = ap[net.c, 0:BLOCK]

    def step(known, k, carry):
        def catch_up(slot, carry):
            pl.when(slot < LAST_W)(lambda: net.wslot(slot))

            @pl.when((slot >= START) & (slot < START + CHUNKS + 5 * SKEW))
            def _():
                net.zslot(slot - START + 1)
                net.qslot(slot - START)

            return carry

        lax.fori_loop(BEFORE + k + jnp.minimum(k, EXTRA), BEFORE + k + 1 + jnp.minimum(k + 1, EXTRA), catch_up, 0)

        @pl.when(k == 0)
        def _():
            net.wtwin(0)
            diag[...] = wb[0, 0]

        if known:
            net.wtwin(k + 1)
            full = slice(0, known)
            x = (xh[full, full], xl[full, full])
            part = split(dot3(x, split(wb[0 : known // BLOCK, k + 1].reshape(known, BLOCK)), NN))
            cross = dot3((colh[full], coll[full]), part, TN)
            square = dot3(part, part, TN)
            across = dot3(part, x, TN)
        inv = split(invert_factor(diag[...]))
        mine = pl.ds(pl.multiple_of(k * BLOCK, BLOCK), BLOCK)
        row = split(-dot3(inv, split(gx[...]), NN))
        xh[mine, :], xl[mine, :] = row
        xh[mine, mine], xl[mine, mine] = inv
        if known:
            last = split(dot3(inv, split(wb[k, k + 1] - cross), NN))
            diag[...] = wb[k + 1, k + 1] - square - dot3(last, last, TN)
            colh[full], coll[full] = part
            colh[mine], coll[mine] = last
            gx[...] = dot3(last, (xh[mine, :], xl[mine, :]), TN)
            gx[:, full] = gx[:, full] + across
        return carry

    lax.fori_loop(0, 5, functools.partial(step, 4 * BLOCK), 0)
    lax.fori_loop(5, 7, functools.partial(step, 6 * BLOCK), 0)
    step(0, jnp.int32(7), 0)
    whole.wait()

    def spread(u, carry):
        for n in range(AFTER):
            slot = BEFORE + STEPS + EXTRA + AFTER * u + n - START
            net.zslot(slot + 1)
            net.qslot(slot)
        for m in range(4):
            pl.when(u > 0)(lambda: net.ztwin(m, 2 * u))
            net.ztwin(m, 2 * u + 1)
        mine = pl.ds(pl.multiple_of(u * WIDE, WIDE), WIDE)
        apu = split(jnp.concatenate([ap[j, mine] for j in range(STEPS)], axis=1))
        aqu = split(jnp.concatenate(
            [jnp.concatenate([aq[i, 2 * u], aq[i, 2 * u + 1]], axis=1) for i in range(STEPS)], axis=0))
        for b in range(ROUNDS):
            lo, hi = b * WIDE, (b + 1) * WIDE
            xb = (xh[lo:hi, :hi], xl[lo:hi, :hi])
            lp = dot3((apu[0][:, :hi], apu[1][:, :hi]), xb, NT)
            lpf[2 * b, mine] = lp[:, :BLOCK]
            lpf[2 * b + 1, mine] = lp[:, BLOCK:]
            lph[u, :, lo:hi], lpl[u, :, lo:hi] = split(lp)
            lqh[u, lo:hi, :], lql[u, lo:hi, :] = split(dot3(xb, (aqu[0][:hi], aqu[1][:hi]), NN))

        def cell(a, b):
            where = (pl.ds(pl.multiple_of(a * WIDE, WIDE), WIDE), pl.ds(pl.multiple_of(b * WIDE, WIDE), WIDE))
            tv[where] = tv[where] - dot3((lph[a], lpl[a]), (lqh[b], lql[b]), NN)

        def cells(v, carry):
            cell(u, v)
            cell(v, u)
            return carry

        lax.fori_loop(0, u, cells, 0)
        cell(u, u)
        return carry

    lax.fori_loop(0, ROUNDS, spread, 0)

    @pl.when(p < STEPS)
    def _():
        tv[0:BLOCK, :] = jnp.zeros((BLOCK, WIDTH), jnp.float32)

    @pl.when(q < STEPS)
    def _():
        tv[BLOCK:, 0:BLOCK] = lpf[q % STEPS, BLOCK:]
        top = lpf[q % STEPS, 0:BLOCK]
        down = lax.broadcasted_iota(jnp.int32, (BLOCK, BLOCK), 0) + p * BLOCK
        across = lax.broadcasted_iota(jnp.int32, (BLOCK, BLOCK), 1) + q * BLOCK
        tv[0:BLOCK, 0:BLOCK] = jnp.where((p >= STEPS) | (down >= across), top, 0.0)

    result = pltpu.make_async_copy(tv, out, osem)
    result.start()
    net.drain()
    result.wait()


def per_device(blocked):
    f32, bf16 = jnp.float32, jnp.bfloat16
    hbm = pl.BlockSpec(memory_space=pl.ANY)
    dma, square = pltpu.SemaphoreType.DMA, (WIDTH, WIDTH)
    return pl.pallas_call(
        kernel,
        name="factor",
        out_shape=jax.ShapeDtypeStruct(square, f32),
        in_specs=[hbm],
        out_specs=hbm,
        scratch_shapes=[
            pltpu.VMEM((STEPS, WIDTH, BLOCK), f32),
            pltpu.VMEM((STEPS, CHUNKS, BLOCK, BLOCK), f32),
            pltpu.VMEM((STEPS, STEPS, BLOCK, BLOCK), f32),
            pltpu.VMEM(square, f32),
            pltpu.VMEM((STEPS, WIDTH, BLOCK), f32),
            *(pltpu.VMEM(square, bf16) for _ in range(2)),
            pltpu.VMEM((BLOCK, WIDTH), f32),
            *(pltpu.VMEM((WIDTH, BLOCK), bf16) for _ in range(2)),
            *(pltpu.VMEM((ROUNDS, WIDE, WIDTH), bf16) for _ in range(2)),
            *(pltpu.VMEM((ROUNDS, WIDTH, WIDE), bf16) for _ in range(2)),
            pltpu.VMEM((BLOCK, BLOCK), f32),
            dma((3 + CHUNKS,)), dma,
            dma((STEPS, CHUNKS)), dma((STEPS, CHUNKS)), dma((STEPS, STEPS)),
        ],
        compiler_params=pltpu.CompilerParams(collective_id=0, has_side_effects=True, vmem_limit_bytes=58 << 20),
    )(blocked)


def solution(mesh):
    return jax.shard_map(
        per_device,
        mesh=mesh,
        in_specs=(P("prow", "pcol"),),
        out_specs=P("prow", "pcol"),
        check_vma=False,
    )
```

```python
import functools

import jax
import jax.numpy as jnp
from jax import lax
from jax.experimental import pallas as pl
from jax.experimental.pallas import tpu as pltpu
from jax.sharding import PartitionSpec as P

BLOCK = 128
STEPS = 8
WIDTH = BLOCK * STEPS
TILE = 8
TILES = BLOCK // TILE
SIDE = 4
RING = 8
CHUNKS = 8
STAGGER = 1
BEFORE = 5
EXTRA = 2
START = 1
AFTER = 1
PASS = (1, 2, 4)
LAST_W = 11
SKEW = 2
WIDE = 2 * BLOCK
ROUNDS = WIDTH // WIDE

UP_FIRST = ((0, 1, 2, 3, 4), (1, 2, 3, 4), (2, 3, 4, 5, 6), (3, 4, 5, 6, 7))
DOWN_FIRST = ((0, 7, 6, 5), (1, 0, 7, 6, 5), (2, 1, 0, 7), (3, 2, 1, 0))
UP = ((0, 1, 2), (1, 2, 3), (2, 3, 4, 5, 6, 7), (3, 4, 5, 6, 7, 0))
DOWN = ((0, 7, 6, 5, 4, 3), (1, 0, 7, 6, 5, 4), (2, 1, 0), (3, 2, 1))


def any_of(value, choices):
    hit = value == choices[0]
    for choice in choices[1:]:
        hit = hit | (value == choice)
    return hit


def table(value, entries):
    out = jnp.int32(entries[0])
    for n, entry in enumerate(entries[1:], 1):
        out = jnp.where(value == n, jnp.int32(entry), out)
    return out


def hops(ups, downs, m):
    return [ups[m].index(z) if z in ups[m] else downs[m].index(z) for z in range(RING)]


class Links:
    def __init__(self, ap, aq, wb, zsem, zsend, qsem, qsend, wsem, wsend, fsend):
        self.ap, self.aq, self.wb = ap, aq, wb
        self.zsem, self.zsend = zsem, zsend
        self.qsem, self.qsend = qsem, qsend
        self.wsem, self.wsend, self.fsend = wsem, wsend, fsend
        self.p, self.q = lax.axis_index("prow"), lax.axis_index("pcol")
        self.y, self.x = self.p // SIDE, self.p % SIDE
        self.z, self.c = self.q // 2, self.q % 2
        self.zhops = [table(self.z, hops(UP, DOWN, m)) for m in range(4)]
        self.zfirst = [table(self.z, hops(UP_FIRST, DOWN_FIRST, m)) for m in range(4)]
        self.up = [any_of(self.z, UP[m][:-1]) for m in range(4)]
        self.down = [any_of(self.z, DOWN[m][:-1]) for m in range(4)]
        self.up_first = [any_of(self.z, UP_FIRST[m][:-1]) for m in range(4)]
        self.down_first = [any_of(self.z, DOWN_FIRST[m][:-1]) for m in range(4)]
        self.beside = (self.device(dy=1), self.device(dy=3), self.device(dx=1), self.device(dx=3))
        self.along = (self.device(dz=1), self.device(dz=RING - 1), self.device(dc=1))
        self.qhops, self.ways = [], []
        for i in range(STEPS):
            ys, dx = i // SIDE, (self.x - i % SIDE + SIDE) % SIDE
            row, same = self.y == ys, dx == 0
            self.qhops.append(table(self.y, (0, 1, 2, 1) if ys == 0 else (1, 0, 1, 2)) + table(dx, (0, 1, 2, 1)))
            turn = row | (self.y == (3 if ys == 0 else 2))
            on = same | (dx == (1 if ys == 0 else 3))
            ways = []
            for down, across in ((same, True), (True, row)):
                one, two = (row & down, turn & down), (on & across, same & across)
                ways.append((*(one if ys == 0 else one[::-1]), *(two if ys == 0 else two[::-1])))
            self.ways.append(ways)

    def device(self, dx=0, dy=0, dz=0, dc=0):
        prow = (self.y + dy) % SIDE * SIDE + (self.x + dx) % SIDE
        pcol = (self.z + dz) % RING * 2 + (self.c + dc) % 2
        return (prow, pcol)

    def neighbours(self):
        around = [self.device(dx=n) for n in (1, 2, 3)] + [self.device(dy=n) for n in (1, 2, 3)]
        return around + [self.device(dz=n) for n in range(1, RING)] + [self.device(dc=1)]

    def copy(self, src, dst, send, recv, device):
        return pltpu.make_async_remote_copy(
            src_ref=src, dst_ref=dst, send_sem=send, recv_sem=recv,
            device_id=device, device_id_type=pl.DeviceIdType.MESH,
        )

    def zcopy(self, way, m, t, parity, first=False):
        j = 2 * m + parity
        part = self.ap.at[j, pl.ds(0 if first else pl.multiple_of(t * BLOCK, BLOCK), BLOCK)]
        return self.copy(part, part, self.zsend.at[int(first), way, m], self.zsem.at[j, t], self.along[way])

    def zitem(self, m, t, first=False):
        up, down = (self.up_first, self.down_first) if first else (self.up, self.down)

        @pl.when(self.z != m)
        def _():
            self.zcopy(0, m, t, self.c, first).wait_recv()

        for way, sends in enumerate((up[m], down[m])):
            @pl.when(sends)
            def _():
                self.zcopy(way, m, t, self.c, first).start()

        self.zcopy(2, m, t, self.c, first).start()

    def zslot(self, slot):
        for m in range(4):
            t = slot - SKEW * self.zhops[m]

            @pl.when((t >= 1) & (t < CHUNKS))
            def _():
                self.zitem(m, t)

    def ztwin(self, m, t, first=False):
        self.zcopy(2, m, t, 1 - self.c, first).wait_recv()

    def qcopy(self, way, i, t, order=0):
        part = self.aq.at[i, t]
        return self.copy(part, part, self.qsend.at[order, way, i], self.qsem.at[i, t], self.beside[way])

    def qslot(self, slot):
        for i in range(STEPS):
            t = slot - SKEW * self.qhops[i]

            @pl.when((t >= 0) & (t < CHUNKS))
            def _():
                @pl.when(self.p != i)
                def _():
                    self.qcopy(0, i, t).wait_recv()

                odd = t % 2
                for way, (even_sends, odd_sends) in enumerate(zip(*self.ways[i])):
                    @pl.when(jnp.where(odd == 1, odd_sends, even_sends))
                    def _():
                        self.qcopy(way, i, t, odd).start()

    def wcopy(self, way, k, m, parity, own=False):
        device = self.along[2] if way == 4 else self.beside[way]
        j = 2 * m + parity
        dst = self.wb.at[k, j]
        src = self.ap.at[j, pl.ds(0, BLOCK)] if own else dst
        send = self.wsend.at[way, m * (m + 1) - 2 + k]
        return self.copy(src, dst, send, self.wsem.at[k, j], device)

    def wneeded(self, k, m):
        return self.c == 1 if k == 2 * m + 1 else self.c >= 0

    def wslot(self, slot):
        for m in range(1, 4):
            for k in range(2 * m + 2):
                @pl.when((self.zfirst[m] + self.qhops[k] + STAGGER * (m - 1) == slot) & self.wneeded(k, m))
                def _():
                    @pl.when(self.p == k)
                    def _():
                        for way in range(4):
                            pl.when(self.ways[k][0][way])(self.wcopy(way, k, m, self.c, own=True).start)

                    @pl.when(self.p != k)
                    def _():
                        self.wcopy(0, k, m, self.c).wait_recv()
                        for way in range(4):
                            pl.when(self.ways[k][0][way])(self.wcopy(way, k, m, self.c).start)
                        self.wcopy(4, k, m, self.c).start()

    def fcopy(self, n, k, parity, own=False):
        if n < 7:
            device = self.device(dz=(4, 3, 5, 2, 6, 1, 7)[n])
        elif n < 13:
            step = (2, 1, 3)[(n - 7) % 3]
            device = self.device(dy=step) if n < 10 else self.device(dx=step)
        else:
            device = self.along[2]
        dst = self.wb.at[k, parity]
        src = self.ap.at[parity, pl.ds(0, BLOCK)] if own else dst
        return self.copy(src, dst, self.fsend.at[n, k], self.wsem.at[k, parity], device)

    def fsource(self):
        for k in range(2):
            @pl.when((self.p == k) & (self.z == 0) & (k <= self.c))
            def _():
                for n in range(14):
                    self.fcopy(n, k, self.c, own=True).start()

    def fpass(self, stage):
        for k in range(2):
            needed = k <= self.c
            if stage == 0:
                here, sends = (self.p == k) & (self.z != 0), range(7, 14)
            elif stage == 1:
                here, sends = (self.x == k) & (self.y != 0), range(10, 14)
            else:
                here, sends = self.x != k, range(13, 14)

            @pl.when(here & needed)
            def _():
                self.fcopy(0, k, self.c).wait_recv()
                for n in sends:
                    self.fcopy(n, k, self.c).start()

    def wtwin(self, j):
        @pl.when(self.c != j % 2)
        def _():
            def item(k, carry):
                part = self.wb.at[k, j]
                twin = self.copy(part, part, self.fsend.at[0, 0], self.wsem.at[k, j], self.along[2])
                pl.when((j < 2) | (self.p != k))(twin.wait_recv)
                return carry

            lax.fori_loop(0, j + 1, item, 0)

    def drain(self):
        for m in range(4):
            for way, first, later in (
                (0, self.up_first[m], self.up[m]), (1, self.down_first[m], self.down[m]), (2, None, None),
            ):
                device = self.device(dc=1)
                one, rest = self.ap.at[0, pl.ds(0, BLOCK)], self.ap.at[0, pl.ds(0, WIDTH - BLOCK)]
                head = self.copy(one, one, self.zsend.at[1, way, m], self.zsem.at[0, 0], device)
                tail = self.copy(rest, rest, self.zsend.at[0, way, m], self.zsem.at[0, 0], device)
                if first is None:
                    head.wait_send()
                    tail.wait_send()
                else:
                    pl.when(first)(head.wait_send)
                    pl.when(later)(tail.wait_send)
        for i in range(STEPS):
            half = self.aq.at[i, pl.ds(0, CHUNKS // 2)]
            for order in range(2):
                for way, sends in enumerate(self.ways[i][order]):
                    every = self.copy(half, half, self.qsend.at[order, way, i], self.qsem.at[0, 0], self.beside[way])
                    pl.when(sends)(every.wait_send)
        for m in range(1, 4):
            for k in range(2 * m + 2):
                for way in range(5):
                    sends = self.ways[k][0][way] if way < 4 else self.p != k
                    pl.when(sends & self.wneeded(k, m))(self.wcopy(way, k, m, self.c).wait_send)
        for k in range(2):
            for n in range(14):
                line = (self.p == k) & (self.z == 0) if n < 7 else self.p == k if n < 10 else self.x == k if n < 13 else True
                pl.when(line & (k <= self.c))(self.fcopy(n, k, self.c).wait_send)


def row_of(x, j):
    return jnp.broadcast_to(x[j : j + 1, :], (TILE, BLOCK))


def lane_of(x, c):
    return jnp.broadcast_to(x[:, c : c + 1], x.shape)


def times(x, n):
    return x if n == 1 else jnp.concatenate([x] * n, axis=0)


def invert_factor(block):
    sub = lax.broadcasted_iota(jnp.int32, (TILE, BLOCK), 0)
    rows = lax.broadcasted_iota(jnp.int32, (BLOCK, BLOCK), 0)
    lanes = lax.broadcasted_iota(jnp.int32, (BLOCK, BLOCK), 1)
    ident = jnp.where(rows == lanes, 1.0, 0.0).astype(jnp.float32)
    head, rest = block[:TILE], block[TILE:]
    bhead, brest = ident[:TILE], ident[TILE:]
    done = []
    ahead = [lane_of(head, j) for j in range(TILE)]
    for s in range(TILES):
        left = TILES - 1 - s
        first = TILE * s
        col = ahead
        if left:
            below = [lane_of(rest, first + j) for j in range(TILE)]
            ahead = [lane_of(rest[:TILE], first + TILE + j) for j in range(TILE)]
        r, b = head, bhead
        scale, coef = [], {}
        for j in range(TILE):
            scale.append(lax.rsqrt(row_of(col[j], j)))
            line = col[j] * scale[j]
            for k in range(j + 1, TILE):
                coef[j, k] = row_of(line, k)
                col[k] = col[k] - line * coef[j, k]
            ru, bu = row_of(r, j) * scale[j], row_of(b, j) * scale[j]
            if j < TILE - 1:
                low = jnp.where(sub > j, line, 0.0)
                r = jnp.where(sub == j, ru, r - low * ru)
                b = jnp.where(sub == j, bu, b - low * bu)
            else:
                r = jnp.where(sub == j, ru, r)
                b = jnp.where(sub == j, bu, b)
        done.append(b)
        if not left:
            break
        lines = []
        for j in range(TILE):
            line = below[j] * times(scale[j], left)
            lines.append(line)
            for k in range(j + 1, TILE):
                below[k] = below[k] - line * times(coef[j, k], left)
        for m in range(TILE):
            near = lines[m][:TILE]
            for j in range(TILE):
                ahead[j] = ahead[j] - near * row_of(near, j)
        for j in range(TILE):
            rest = rest - lines[j] * times(row_of(r, j), left)
            brest = brest - lines[j] * times(row_of(b, j), left)
        head, bhead = rest[:TILE], brest[:TILE]
        if left > 1:
            rest, brest = rest[TILE:], brest[TILE:]
    return jnp.concatenate(done, axis=0)


def split(x):
    high = x.astype(jnp.bfloat16)
    return high, (x - high.astype(jnp.float32)).astype(jnp.bfloat16)


NN = (((1,), (0,)), ((), ()))
TN = (((0,), (0,)), ((), ()))
NT = (((1,), (1,)), ((), ()))


def dot3(a, b, dims):
    one = functools.partial(lax.dot_general, dimension_numbers=dims, preferred_element_type=jnp.float32)
    return one(a[0], b[0]) + one(a[0], b[1]) + one(a[1], b[0])


def kernel(t_ref, out, ap, aq, wb, tv, lpf, xh, xl, gx, colh, coll, lph, lpl, lqh, lql, diag, lsem, osem, zsem, qsem, wsem):
    dma = pltpu.SemaphoreType.DMA
    pl.run_scoped(
        functools.partial(steps, t_ref, out, ap, aq, wb, tv, lpf, xh, xl, gx, colh, coll, lph, lpl, lqh, lql, diag, lsem, osem, zsem, qsem, wsem),
        dma((2, 3, 4)), dma((2, 4, STEPS)), dma((5, 18)), dma((14, 2)),
    )


def steps(
    t_ref, out, ap, aq, wb, tv, lpf, xh, xl, gx, colh, coll, lph, lpl, lqh, lql, diag, lsem, osem, zsem, qsem, wsem,
    zsend, qsend, wsend, fsend,
):
    net = Links(ap, aq, wb, zsem, zsend, qsem, qsend, wsem, wsend, fsend)
    p, q = net.p, net.q
    barrier = pltpu.get_barrier_semaphore()
    for device in net.neighbours():
        pl.semaphore_signal(barrier, inc=1, device_id=device, device_id_type=pl.DeviceIdType.MESH)
    cols = pl.ds(0, BLOCK)
    head = pltpu.make_async_copy(t_ref.at[cols, cols], ap.at[q % STEPS, cols], lsem.at[0])
    later = pl.ds(BLOCK, WIDTH - BLOCK)
    body = pltpu.make_async_copy(t_ref.at[later, cols], ap.at[q % STEPS, later], lsem.at[1])
    rows = [
        pltpu.make_async_copy(t_ref.at[cols, pl.ds(t * BLOCK, BLOCK)], aq.at[p % STEPS, t], lsem.at[2 + t])
        for t in range(CHUNKS)
    ]
    whole = pltpu.make_async_copy(t_ref, tv, lsem.at[2 + CHUNKS])

    @pl.when(q < STEPS)
    def _():
        head.start()
        body.start()

    @pl.when(p < STEPS)
    def _():
        for row in rows:
            row.start()

    whole.start()
    xh[...] = jnp.zeros_like(xh)
    xl[...] = jnp.zeros_like(xl)
    gx[...] = jnp.zeros_like(gx)
    colh[...] = jnp.zeros_like(colh)
    coll[...] = jnp.zeros_like(coll)

    for k in range(1, STEPS):
        for j in range(k):
            wb[k, j] = jnp.zeros((BLOCK, BLOCK), jnp.float32)

    pl.semaphore_wait(barrier, 14)

    @pl.when(q < STEPS)
    def _():
        head.wait()
        body.wait()

    @pl.when(p < STEPS)
    def _():
        for row in rows:
            row.wait()

    net.fsource()

    def first(slot, carry):
        for m in range(4):
            pl.when(net.zfirst[m] == slot)(functools.partial(net.zitem, m, 0, True))
        net.wslot(slot)
        net.zslot(slot - START + 1)
        net.qslot(slot - START)
        for stage, at in enumerate(PASS):
            pl.when(slot == at)(functools.partial(net.fpass, stage))
        return carry

    lax.fori_loop(0, BEFORE, first, 0)
    for m in range(4):
        net.ztwin(m, 0, first=True)
    for k in range(STEPS):
        @pl.when(p == k)
        def _():
            for j in range(max(k, 2), STEPS):
                wb[k, j] = ap[j, 0:BLOCK]

    for k in range(2):
        @pl.when((p == k) & (net.z == 0) & (k <= net.c))
        def _():
            wb[k, net.c] = ap[net.c, 0:BLOCK]

    def step(known, k, carry):
        def catch_up(slot, carry):
            pl.when(slot < LAST_W)(lambda: net.wslot(slot))

            @pl.when((slot >= START) & (slot < START + CHUNKS + 5 * SKEW))
            def _():
                net.zslot(slot - START + 1)
                net.qslot(slot - START)

            return carry

        lax.fori_loop(BEFORE + k + jnp.minimum(k, EXTRA), BEFORE + k + 1 + jnp.minimum(k + 1, EXTRA), catch_up, 0)

        @pl.when(k == 0)
        def _():
            net.wtwin(0)
            diag[...] = wb[0, 0]

        if known:
            net.wtwin(k + 1)
            full = slice(0, known)
            x = (xh[full, full], xl[full, full])
            part = split(dot3(x, split(wb[0 : known // BLOCK, k + 1].reshape(known, BLOCK)), NN))
            cross = dot3((colh[full], coll[full]), part, TN)
            square = dot3(part, part, TN)
            across = dot3(part, x, TN)
        inv = split(invert_factor(diag[...]))
        mine = pl.ds(pl.multiple_of(k * BLOCK, BLOCK), BLOCK)
        row = split(-dot3(inv, split(gx[...]), NN))
        xh[mine, :], xl[mine, :] = row
        xh[mine, mine], xl[mine, mine] = inv
        if known:
            last = split(dot3(inv, split(wb[k, k + 1] - cross), NN))
            diag[...] = wb[k + 1, k + 1] - square - dot3(last, last, TN)
            colh[full], coll[full] = part
            colh[mine], coll[mine] = last
            gx[...] = dot3(last, (xh[mine, :], xl[mine, :]), TN)
            gx[:, full] = gx[:, full] + across
        return carry

    lax.fori_loop(0, 5, functools.partial(step, 4 * BLOCK), 0)
    lax.fori_loop(5, 7, functools.partial(step, 6 * BLOCK), 0)
    step(0, jnp.int32(7), 0)
    whole.wait()

    def spread(u, carry):
        for n in range(AFTER):
            slot = BEFORE + STEPS + EXTRA + AFTER * u + n - START
            net.zslot(slot + 1)
            net.qslot(slot)
        for m in range(4):
            pl.when(u > 0)(lambda: net.ztwin(m, 2 * u))
            net.ztwin(m, 2 * u + 1)
        mine = pl.ds(pl.multiple_of(u * WIDE, WIDE), WIDE)
        apu = split(jnp.concatenate([ap[j, mine] for j in range(STEPS)], axis=1))
        aqu = split(jnp.concatenate(
            [jnp.concatenate([aq[i, 2 * u], aq[i, 2 * u + 1]], axis=1) for i in range(STEPS)], axis=0))
        for b in range(ROUNDS):
            lo, hi = b * WIDE, (b + 1) * WIDE
            xb = (xh[lo:hi, :hi], xl[lo:hi, :hi])
            lp = dot3((apu[0][:, :hi], apu[1][:, :hi]), xb, NT)
            lpf[2 * b, mine] = lp[:, :BLOCK]
            lpf[2 * b + 1, mine] = lp[:, BLOCK:]
            lph[u, :, lo:hi], lpl[u, :, lo:hi] = split(lp)
            lqh[u, lo:hi, :], lql[u, lo:hi, :] = split(dot3(xb, (aqu[0][:hi], aqu[1][:hi]), NN))

        def cell(a, b):
            where = (pl.ds(pl.multiple_of(a * WIDE, WIDE), WIDE), pl.ds(pl.multiple_of(b * WIDE, WIDE), WIDE))
            tv[where] = tv[where] - dot3((lph[a], lpl[a]), (lqh[b], lql[b]), NN)

        def cells(v, carry):
            cell(u, v)
            cell(v, u)
            return carry

        lax.fori_loop(0, u, cells, 0)
        cell(u, u)
        return carry

    lax.fori_loop(0, ROUNDS, spread, 0)

    @pl.when(p < STEPS)
    def _():
        tv[0:BLOCK, :] = jnp.zeros((BLOCK, WIDTH), jnp.float32)

    @pl.when(q < STEPS)
    def _():
        tv[BLOCK:, 0:BLOCK] = lpf[q % STEPS, BLOCK:]
        top = lpf[q % STEPS, 0:BLOCK]
        down = lax.broadcasted_iota(jnp.int32, (BLOCK, BLOCK), 0) + p * BLOCK
        across = lax.broadcasted_iota(jnp.int32, (BLOCK, BLOCK), 1) + q * BLOCK
        tv[0:BLOCK, 0:BLOCK] = jnp.where((p >= STEPS) | (down >= across), top, 0.0)

    result = pltpu.make_async_copy(tv, out, osem)
    result.start()
    net.drain()
    result.wait()


def per_device(blocked):
    f32, bf16 = jnp.float32, jnp.bfloat16
    hbm = pl.BlockSpec(memory_space=pl.ANY)
    dma, square = pltpu.SemaphoreType.DMA, (WIDTH, WIDTH)
    return pl.pallas_call(
        kernel,
        name="factor",
        out_shape=jax.ShapeDtypeStruct(square, f32),
        in_specs=[hbm],
        out_specs=hbm,
        scratch_shapes=[
            pltpu.VMEM((STEPS, WIDTH, BLOCK), f32),
            pltpu.VMEM((STEPS, CHUNKS, BLOCK, BLOCK), f32),
            pltpu.VMEM((STEPS, STEPS, BLOCK, BLOCK), f32),
            pltpu.VMEM(square, f32),
            pltpu.VMEM((STEPS, WIDTH, BLOCK), f32),
            *(pltpu.VMEM(square, bf16) for _ in range(2)),
            pltpu.VMEM((BLOCK, WIDTH), f32),
            *(pltpu.VMEM((WIDTH, BLOCK), bf16) for _ in range(2)),
            *(pltpu.VMEM((ROUNDS, WIDE, WIDTH), bf16) for _ in range(2)),
            *(pltpu.VMEM((ROUNDS, WIDTH, WIDE), bf16) for _ in range(2)),
            pltpu.VMEM((BLOCK, BLOCK), f32),
            dma((3 + CHUNKS,)), dma,
            dma((STEPS, CHUNKS)), dma((STEPS, CHUNKS)), dma((STEPS, STEPS)),
        ],
        compiler_params=pltpu.CompilerParams(collective_id=0, has_side_effects=True, vmem_limit_bytes=58 << 20),
    )(blocked)


def solution(mesh):
    return jax.shard_map(
        per_device,
        mesh=mesh,
        in_specs=(P("prow", "pcol"),),
        out_specs=P("prow", "pcol"),
        check_vma=False,
    )
```
